32 devices in a mesh: dp: 4 (over x, y), sp: 8 (over z, core).
Axes of the slice: x: 2, y: 2, z: 4, core: 2. Of those that a mesh axis runs over, the one named last changes fastest.
Arguments:
- x: bfloat16 [16384, 3072], P(('dp', 'sp')), parts along dimension 0
- gain: bfloat16 [3072], replicated
- wq: bfloat16 [3072, 3072], replicated
- wk: bfloat16 [3072, 1024], replicated
- wv: bfloat16 [3072, 1024], replicated
- wo: bfloat16 [3072, 3072], replicated
Outputs:
- output: bfloat16 [16384, 3072], P(('dp', 'sp')), parts along dimension 0
There are 4 independent parts. The reference program is written for one: setup_inputs(seed, part) draws one part's arguments, and reference() takes and returns one part's arrays. A program takes and returns all parts, laid end to end along the dimension named above; an argument that names none is the same for every part.
All inputs are finite; a program needn't handle non-finite values.
Results may differ from the reference program's by a relative error of at most 0.012.
Values are sent between devices in bfloat16 or wider.
A program may use at most 2 GiB of HBM per device.

```python
import jax
import jax.numpy as jnp
from jax import lax

ROWS = 4096
D = 3072
HEADS = 24
KV_HEADS = 8
HEAD = 128
THETA = 10000


def setup_inputs(seed: int = 0, part: int = 0) -> dict:
    kx, kn, kq, kk, kv, ko = jax.random.split(jax.random.key(seed), 6)

    def weights(key, rows, columns):
        return jax.random.normal(key, (rows, columns), jnp.float32) * rows**-0.5

    drawn = {
        "x": jax.random.normal(jax.random.fold_in(kx, part), (ROWS, D), jnp.float32),
        "gain": 1 + 0.1 * jax.random.normal(kn, (D,), jnp.float32),
        "wq": 2 * weights(kq, D, HEADS * HEAD),
        "wk": 2 * weights(kk, D, KV_HEADS * HEAD),
        "wv": 4 * weights(kv, D, KV_HEADS * HEAD),
        "wo": weights(ko, HEADS * HEAD, D),
    }
    return {k: v.astype(jnp.bfloat16) for k, v in drawn.items()}


def normed(x, gain):
    wide = x.astype(jnp.float32)
    scale = lax.rsqrt(jnp.mean(wide * wide, -1, keepdims=True) + 1e-6)
    return (wide * scale * gain.astype(jnp.float32)).astype(jnp.bfloat16)


def turned(t, place, theta):
    half = t.shape[-1] // 2
    angle = place.astype(jnp.float32)[:, None] * theta ** (-jnp.arange(half, dtype=jnp.float32) / half)
    cos, sin = jnp.cos(angle)[:, None], jnp.sin(angle)[:, None]
    a, b = t[..., :half].astype(jnp.float32), t[..., half:].astype(jnp.float32)
    return jnp.concatenate([a * cos - b * sin, b * cos + a * sin], -1).astype(jnp.bfloat16)


def matmul(a, w):
    return jnp.dot(a, w, preferred_element_type=jnp.float32).astype(jnp.bfloat16)


def einsum(form, a, b):
    return jnp.einsum(form, a.astype(jnp.float32), b.astype(jnp.float32))


def attention(q, k, v):
    scores = einsum("tgsd,ugd->gstu", q, k) * q.shape[-1] ** -0.5
    token = jnp.arange(q.shape[0])
    scores = jnp.where(token[:, None] >= token, scores, -jnp.inf)
    weights = jax.nn.softmax(scores, -1).astype(jnp.bfloat16)
    return einsum("gstu,ugd->tgsd", weights, v).astype(jnp.bfloat16)


def reference(x, gain, wq, wk, wv, wo):
    a, place = normed(x, gain), jnp.arange(ROWS)
    q = turned(matmul(a, wq).reshape(ROWS, HEADS, HEAD), place, THETA).reshape(ROWS, KV_HEADS, -1, HEAD)
    k = turned(matmul(a, wk).reshape(ROWS, KV_HEADS, HEAD), place, THETA)
    v = matmul(a, wv).reshape(ROWS, KV_HEADS, HEAD)
    seen = attention(q, k, v).reshape(ROWS, HEADS * HEAD)
    return (x.astype(jnp.float32) + jnp.dot(seen, wo, preferred_element_type=jnp.float32)).astype(jnp.bfloat16)
```

```python
import functools

import jax
import jax.numpy as jnp
from jax import lax
from jax.experimental import pallas as pl
from jax.experimental.pallas import tpu as pltpu
from jax.sharding import PartitionSpec as P

HEAD = 128
THETA = 10000
NEG = -1e30
HIDDEN = 2 * NEG
LOG2E = 1.4426950408889634
E = HEAD**-0.5 * LOG2E
VMEM = 63 * 2**20
BACK = 3
CHIPS = 4
CORES = 2
SP = CHIPS * CORES
F32, BF16 = jnp.float32, jnp.bfloat16


def _dot(a, b, ca, cb):
    return lax.dot_general(a, b, (((ca,), (cb,)), ((), ())), preferred_element_type=F32)


def _kernel(x_ref, gain_ref, cos_ref, sin_ref, wq_ref, wk_ref, wv_ref, wo_ref, y_ref,
            x_s, a_s, wkv_s, wq_s, wo_s, kv, q_s, q3, o3, st3, y_s, o_s, top_s, mix_s,
            x_sem, wkv_sem, wq_sem, wo_sem, y_sem, send_sem, recv_sem, qsend_sem, qrecv_sem, osend_sem, orecv_sem,
            *, kv_heads, group):
    T, D = x_s.shape
    gw = group * HEAD
    me = lax.axis_index("sp")
    chip, core = me // CORES, me % CORES
    other = me + 1 - 2 * core
    last, before = CHIPS - 1, CHIPS - 2

    def is_back(g):
        return (g % 2 == 1) & (g < 2 * BACK)

    def w_kv(g, slot):
        at = pl.ds(pl.multiple_of(g * HEAD, HEAD), HEAD)
        return (pltpu.make_async_copy(wk_ref.at[:, at], wkv_s.at[slot, :, pl.ds(0, HEAD)], wkv_sem.at[slot, 0]),
                pltpu.make_async_copy(wv_ref.at[:, at], wkv_s.at[slot, :, pl.ds(HEAD, HEAD)], wkv_sem.at[slot, 1]))

    def w_q(g, slot):
        return pltpu.make_async_copy(wq_ref.at[:, pl.ds(pl.multiple_of(g * gw, HEAD), gw)], wq_s.at[slot], wq_sem.at[slot])

    def w_o(g, slot):
        return pltpu.make_async_copy(wo_ref.at[pl.ds(pl.multiple_of(g * gw, HEAD), gw), :], wo_s.at[slot], wo_sem.at[slot])

    def piece(g, src, kind, target):
        return pltpu.make_async_remote_copy(src_ref=kv.at[g, src], dst_ref=kv.at[g, src], send_sem=send_sem.at[kind, g, src],
                                            recv_sem=recv_sem.at[g, src], device_id={"sp": target})

    def got(g, src):
        piece(g, src, 0, other).wait_recv()

    def query_back(g):
        i = g // 2
        return pltpu.make_async_remote_copy(src_ref=q_s.at[g], dst_ref=q3.at[i], send_sem=qsend_sem.at[i], recv_sem=qrecv_sem.at[i],
                                            device_id={"sp": me - CORES})

    def result_back(i, target):
        return (pltpu.make_async_remote_copy(src_ref=o3.at[i], dst_ref=o3.at[i], send_sem=osend_sem.at[0, i],
                                             recv_sem=orecv_sem.at[0, i], device_id={"sp": target}),
                pltpu.make_async_remote_copy(src_ref=st3.at[i], dst_ref=st3.at[i], send_sem=osend_sem.at[1, i],
                                             recv_sem=orecv_sem.at[1, i], device_id={"sp": target}))

    def sends_own(g, do):
        do(lambda: piece(g, me, 0, other), None)
        do(lambda: piece(g, me, 1, me + CORES), (chip < before) | ((chip == before) & jnp.logical_not(is_back(g))))
        do(lambda: piece(g, me, 2, me + 2 * CORES), chip == 0)

    def sends_on(g, src, do):
        do(lambda: piece(g, src, 0, other), None)
        do(lambda: piece(g, src, 1, me + CORES), (chip == before) & jnp.logical_not(is_back(g)))

    def start(copy, cond):
        if cond is None:
            copy().start()
        else:
            pl.when(cond)(lambda: copy().start())

    def finish(copy, cond):
        if cond is None:
            copy().wait_send()
        else:
            pl.when(cond)(lambda: copy().wait_send())

    pltpu.make_async_copy(x_ref, x_s, x_sem).start()
    for c in w_kv(0, 0):
        c.start()
    barrier = pltpu.get_barrier_semaphore()
    for d in range(1, SP):
        pl.semaphore_signal(barrier, inc=1, device_id={"sp": lax.rem(me + d, SP)})
    for c in w_kv(1, 1):
        c.start()
    w_q(0, 0).start()
    w_q(1, 1).start()
    pltpu.make_async_copy(x_ref, x_s, x_sem).wait()
    rows = min(T, 64)

    def norm(i, _):
        at = pl.ds(pl.multiple_of(i * rows, rows), rows)
        wide = x_s[at, :].astype(F32)
        scale = lax.rsqrt(jnp.mean(wide * wide, -1, keepdims=True) + 1e-6)
        a_s[at, :] = (wide * scale * gain_ref[...].astype(F32)).astype(BF16)
        y_s[at, :] = wide
        return 0

    lax.fori_loop(0, T // rows, norm, 0)
    pl.semaphore_wait(barrier, SP - 1)

    def turned(t):
        t = t.astype(BF16).astype(F32)
        return (t * cos_ref[...] + pltpu.roll(t, HEAD // 2, 1) * sin_ref[...]).astype(BF16)

    def project_kv(g, _):
        slot = g % 2
        for c in w_kv(g, slot):
            c.wait()
        r = _dot(a_s[...], wkv_s[slot], 1, 0)
        kv[g, me, 0] = turned(r[:, :HEAD])
        vt = r[:, HEAD:].T.astype(BF16)
        for n in range(T // HEAD):
            kv[g, me, 1, n * HEAD : (n + 1) * HEAD, :] = vt[:, n * HEAD : (n + 1) * HEAD]

        @pl.when(g + 2 < kv_heads)
        def _():
            for c in w_kv(g + 2, slot):
                c.start()

        sends_own(g, start)
        return 0

    lax.fori_loop(0, kv_heads, project_kv, 0)
    w_o(0, 0).start()
    w_o(1, 1).start()

    def project_q(g, _):
        slot = g % 2
        w_q(g, slot).wait()
        r = _dot(a_s[...], wq_s[slot], 1, 0)
        for i in range(group):
            q_s[g, i] = turned(r[:, i * HEAD : (i + 1) * HEAD])

        @pl.when(g + 2 < kv_heads)
        def _():
            w_q(g + 2, slot).start()

        @pl.when((chip == last) & is_back(g))
        def _():
            query_back(g).start()

        return 0

    lax.fori_loop(0, kv_heads, project_q, 0)

    def clear():
        top_s[...] = jnp.full(top_s.shape, NEG, F32)
        mix_s[...] = jnp.zeros(mix_s.shape, F32)

    def block(q, g, src, masked):
        keys = kv[g, src, 0]
        values = jnp.concatenate([kv[g, src, 1, n * HEAD : (n + 1) * HEAD, :] for n in range(T // HEAD)], axis=1)
        values = jnp.concatenate([values, jnp.ones((8, T), BF16)], axis=0)
        scores = [_dot(keys, q[i], 1, 1) for i in range(group)]
        if masked:
            ok = lax.broadcasted_iota(jnp.int32, (T, T), 1) >= lax.broadcasted_iota(jnp.int32, (T, T), 0)
        weights, keeps = [], []
        for i, s in enumerate(scores):
            if masked:
                s = jnp.where(ok, s, HIDDEN)
            old = top_s[i : i + 1, :]
            top = jnp.maximum(old, s.max(axis=0, keepdims=True))
            top_s[i : i + 1, :] = top
            weights.append(jnp.exp2((s - top) * E).astype(BF16))
            keeps.append(jnp.exp2((old - top) * E))
        for i, (p, keep) in enumerate(zip(weights, keeps)):
            mix_s[i] = mix_s[i] * keep + _dot(values, p, 1, 0)

    def attend(g, _):
        slot = g % 2
        back = is_back(g)
        clear()
        block(q_s.at[g], g, me, True)
        got(g, other)

        @pl.when(core == 1)
        def _():
            block(q_s.at[g], g, other, False)

        def remote(j, _):
            half = lax.rem(core + j, CORES)
            src = (chip - 1 - j // CORES) * CORES + half
            got(g, src)

            @pl.when(half == core)
            def _():
                sends_on(g, src, start)

            block(q_s.at[g], g, src, False)
            return 0

        lax.fori_loop(0, jnp.where((chip == last) & back, 0, chip * CORES), remote, 0)

        @pl.when((chip == last) & back)
        def _():
            i3 = g // 2
            for c in result_back(i3, me - CORES):
                c.wait_recv()
            for i in range(group):
                mine, theirs = top_s[i : i + 1, :], st3[i3, i : i + 1, :]
                top = jnp.maximum(mine, theirs)
                a = jnp.exp2((mine - top) * E)
                b = jnp.exp2((theirs - top) * E) * st3[i3, 8 + i : 9 + i, :]
                mix_s[i, :HEAD, :] = mix_s[i, :HEAD, :] * a + o3[i3, i].astype(F32) * b
                mix_s[i, HEAD:, :] = mix_s[i, HEAD:, :] * a + b

        for i in range(group):
            total = mix_s[i, HEAD : HEAD + 1, :]
            o_s[:, i * HEAD : (i + 1) * HEAD] = (mix_s[i, :HEAD, :] * (1 / total)).T.astype(BF16)

        @pl.when((chip == before) & back)
        def _():
            i3 = g // 2
            query_back(g).wait_recv()
            clear()

            def remote3(j, _):
                block(q3.at[i3], g, j, False)
                return 0

            lax.fori_loop(0, last * CORES, remote3, 0)
            st3[i3, 0:8, :] = top_s[...]
            for i in range(group):
                total = mix_s[i, HEAD : HEAD + 1, :]
                st3[i3, 8 + i : 9 + i, :] = total
                o3[i3, i] = (mix_s[i, :HEAD, :] * (1 / total)).astype(BF16)
            for c in result_back(i3, me + CORES):
                c.start()

        w_o(g, slot).wait()
        wide = min(D, 512)
        for n in range(0, D, wide):
            y_s[:, n : n + wide] += _dot(o_s[...], wo_s[slot, :, n : n + wide], 1, 0)

        @pl.when(g + 2 < kv_heads)
        def _():
            w_o(g + 2, slot).start()

        return 0

    lax.fori_loop(0, kv_heads, attend, 0)

    def out(i, _):
        at = pl.ds(pl.multiple_of(i * rows, rows), rows)
        a_s[at, :] = y_s[at, :].astype(BF16)
        return 0

    lax.fori_loop(0, T // rows, out, 0)
    copy = pltpu.make_async_copy(a_s, y_ref, y_sem)
    copy.start()

    def drain(g, _):
        sends_own(g, finish)

        def on(e, _):
            sends_on(g, e * CORES + core, finish)
            return 0

        lax.fori_loop(0, jnp.where((chip == last) & is_back(g), 0, chip), on, 0)

        @pl.when((chip == last) & is_back(g))
        def _():
            query_back(g).wait_send()

        @pl.when((chip == before) & is_back(g))
        def _():
            for c in result_back(g // 2, me + CORES):
                c.wait_send()

        return 0

    lax.fori_loop(0, kv_heads, drain, 0)
    copy.wait()


def layer(x, gain, cos, sin, wq, wk, wv, wo):
    T, D = x.shape
    kv_heads = wk.shape[1] // HEAD
    group = wq.shape[1] // wk.shape[1]
    gw = group * HEAD
    nb = max(BACK, 1)
    dma = pltpu.SemaphoreType.DMA
    hbm, vmem = pl.BlockSpec(memory_space=pl.ANY), pl.BlockSpec(memory_space=pltpu.VMEM)
    flops = 2 * T * D * (2 * wq.shape[1] + 2 * wk.shape[1]) + 4 * T * T * SP * wq.shape[1] // 2
    return pl.pallas_call(
        functools.partial(_kernel, kv_heads=kv_heads, group=group),
        out_shape=jax.ShapeDtypeStruct((T, D), BF16),
        in_specs=[hbm, vmem, vmem, vmem, hbm, hbm, hbm, hbm],
        out_specs=hbm,
        scratch_shapes=[
            pltpu.VMEM((T, D), BF16),
            pltpu.VMEM((T, D), BF16),
            pltpu.VMEM((2, D, 2 * HEAD), BF16),
            pltpu.VMEM((2, D, gw), BF16),
            pltpu.VMEM((2, gw, D), BF16),
            pltpu.VMEM((kv_heads, SP, 2, T, HEAD), BF16),
            pltpu.VMEM((kv_heads, group, T, HEAD), BF16),
            pltpu.VMEM((nb, group, T, HEAD), BF16),
            pltpu.VMEM((nb, group, HEAD, T), BF16),
            pltpu.VMEM((nb, 16, T), F32),
            pltpu.VMEM((T, D), F32),
            pltpu.VMEM((T, gw), BF16),
            pltpu.VMEM((8, T), F32),
            pltpu.VMEM((group, HEAD + 8, T), F32),
            dma, dma((2, 2)), dma((2,)), dma((2,)), dma,
            dma((3, kv_heads, SP)), dma((kv_heads, SP)), dma((nb,)), dma((nb,)), dma((2, nb)), dma((2, nb)),
        ],
        compiler_params=pltpu.CompilerParams(collective_id=0, has_side_effects=True, vmem_limit_bytes=VMEM),
        cost_estimate=pl.CostEstimate(flops=flops, transcendentals=T * T * SP * wq.shape[1] // HEAD, bytes_accessed=60 * 2**20),
    )(x, gain.reshape(1, D), cos, sin, wq, wk, wv, wo)


def solution(mesh):
    def step(x, gain, wq, wk, wv, wo):
        own, half = x.shape[0], HEAD // 2
        place = lax.axis_index("sp") * own + jnp.arange(own)
        angle = place.astype(F32)[:, None] * THETA ** (-jnp.arange(half, dtype=F32) / half)
        cos, sin = jnp.cos(angle), jnp.sin(angle)
        return layer(x, gain, jnp.concatenate([cos, cos], 1), jnp.concatenate([-sin, sin], 1), wq, wk, wv, wo)

    tokens, whole = P(("dp", "sp"), None), P(None, None)
    return jax.shard_map(
        step,
        mesh=mesh,
        in_specs=(tokens, P(None), whole, whole, whole, whole),
        out_specs=tokens,
        check_vma=False,
    )
```

```python
import functools

import jax
import jax.numpy as jnp
import numpy as np
from jax import lax
from jax.experimental import pallas as pl
from jax.experimental.pallas import tpu as pltpu
from jax.sharding import PartitionSpec as P

HEAD = 128
THETA = 10000
NEG = -1e30
HIDDEN = 2 * NEG
LOG2E = 1.4426950408889634
E = HEAD**-0.5 * LOG2E
VMEM = 60 * 2**20
BACK = (0, 2, 4)
ORDER = (1, 3, 0, 5, 2, 6, 4, 7)
AHEAD = 1
STRIP = 256
CHIPS = 4
CORES = 2
SP = CHIPS * CORES
F32, BF16 = jnp.float32, jnp.bfloat16


def _dot(a, b, ca, cb):
    return lax.dot_general(a, b, (((ca,), (cb,)), ((), ())), preferred_element_type=F32)


def _kernel(x_ref, gain_ref, base_ref, cos_ref, sin_ref, wq_ref, wk_ref, wv_ref, wo_ref, y_ref,
            xq_s, a_s, gain_s, cos_s, sin_s, wkv_s, w_s, kv, q3, o3, st3, y_s, o_s, top_s, mix_s,
            x_sem, rope_sem, wkv_sem, w_sem, send_sem, recv_sem, qsend_sem, qrecv_sem, osend_sem, orecv_sem,
            *, kv_heads, group):
    T, D = xq_s.shape
    gw = group * HEAD
    pw = 2 * gw
    pairs = kv_heads // 2
    me = lax.axis_index("sp")
    chip, core = me // CORES, me % CORES
    other = me + 1 - 2 * core
    last, before = CHIPS - 1, CHIPS - 2

    def is_back(g):
        found = g == BACK[0]
        for b in BACK[1:]:
            found = found | (g == b)
        return found

    def back_index(g):
        return sum((g > b).astype(jnp.int32) for b in BACK)

    parts = 4
    rows = T // parts

    def x_part(i):
        at = pl.ds(i * rows, rows)
        return pltpu.make_async_copy(x_ref.at[at, :], xq_s.at[at, :], x_sem.at[i])

    def ropes():
        return (pltpu.make_async_copy(cos_ref, cos_s, rope_sem.at[0]), pltpu.make_async_copy(sin_ref, sin_s, rope_sem.at[1]))

    def w_kv(g, slot):
        at = pl.ds(pl.multiple_of(g * HEAD, HEAD), HEAD)
        return (pltpu.make_async_copy(wk_ref.at[:, at], wkv_s.at[slot, :, pl.ds(0, HEAD)], wkv_sem.at[slot, 0]),
                pltpu.make_async_copy(wv_ref.at[:, at], wkv_s.at[slot, :, pl.ds(HEAD, HEAD)], wkv_sem.at[slot, 1]))

    def w_q(p, slot):
        return (pltpu.make_async_copy(wq_ref.at[:, pl.ds(pl.multiple_of(p * pw, HEAD), pw)], w_s.at[slot, pl.ds(0, D)],
                                      w_sem.at[slot, 0]),)

    wide = D // 4

    def head_of(t):
        mine = sum(jnp.where(t == n, g, 0) for n, g in enumerate(ORDER))
        return jnp.where(chip == last, mine, t)

    def w_o(p, slot):
        at = [pl.ds(pl.multiple_of(head_of(2 * p + h) * gw, HEAD), gw) for h in range(2)]
        return [pltpu.make_async_copy(wo_ref.at[at[h], pl.ds(n * wide, wide)],
                                      w_s.at[slot, pl.ds(n * pw + h * gw, gw), pl.ds(0, wide)], w_sem.at[slot, 4 * h + n])
                for h in range(2) for n in range(4)]

    def piece(g, src, kind, target):
        return pltpu.make_async_remote_copy(src_ref=kv.at[g, src], dst_ref=kv.at[g, src], send_sem=send_sem.at[kind, g, src],
                                            recv_sem=recv_sem.at[g, src], device_id={"sp": target})

    def got(g, src):
        piece(g, src, 0, other).wait_recv()

    def q_at(g):
        return pl.ds(pl.multiple_of(g * gw, HEAD), gw)

    def query_back(g):
        i = back_index(g)
        return pltpu.make_async_remote_copy(src_ref=xq_s.at[:, q_at(g)], dst_ref=q3.at[i], send_sem=qsend_sem.at[i],
                                            recv_sem=qrecv_sem.at[i], device_id={"sp": me - CORES})

    def result_back(i, target):
        return (pltpu.make_async_remote_copy(src_ref=o3.at[i], dst_ref=o3.at[i], send_sem=osend_sem.at[0, i],
                                             recv_sem=orecv_sem.at[0, i], device_id={"sp": target}),
                pltpu.make_async_remote_copy(src_ref=st3.at[i], dst_ref=st3.at[i], send_sem=osend_sem.at[1, i],
                                             recv_sem=orecv_sem.at[1, i], device_id={"sp": target}))

    def sends_own(g, do):
        do(lambda: piece(g, me, 0, other), None)
        do(lambda: piece(g, me, 1, me + CORES), (chip < before) | ((chip == before) & jnp.logical_not(is_back(g))))
        do(lambda: piece(g, me, 2, me + 2 * CORES), chip == 0)

    def sends_on(g, src, do):
        do(lambda: piece(g, src, 0, other), None)
        do(lambda: piece(g, src, 1, me + CORES), (chip == before) & jnp.logical_not(is_back(g)))

    def start(copy, cond):
        if cond is None:
            copy().start()
        else:
            pl.when(cond)(lambda: copy().start())

    def finish(copy, cond):
        if cond is None:
            copy().wait_send()
        else:
            pl.when(cond)(lambda: copy().wait_send())

    for i in range(parts):
        x_part(i).start()
    barrier = pltpu.get_barrier_semaphore()
    for d in range(1, SP):
        pl.semaphore_signal(barrier, inc=1, device_id={"sp": lax.rem(me + d, SP)})
    for c in (*w_kv(0, 0), *ropes(), *w_kv(1, 1)):
        c.start()
    for n in range(D // HEAD):
        gain_s[:, n * HEAD : (n + 1) * HEAD] = gain_ref[n : n + 1, :].astype(F32)
    for i in range(parts):
        with jax.named_scope("waitx"):
            x_part(i).wait()
        step = min(rows, 64)
        for at in range(i * rows, (i + 1) * rows, step):
            x = xq_s[at : at + step, :].astype(F32)
            scale = lax.rsqrt(jnp.mean(x * x, -1, keepdims=True) + 1e-6)
            a_s[at : at + step, :] = (x * scale * gain_s[...]).astype(BF16)
            y_s[at : at + step, :] = x
    with jax.named_scope("rope"):
        for c in ropes():
            c.wait()
        cb, sb = base_ref[pl.ds(me, 1), :], base_ref[pl.ds(SP + me, 1), :]
        cr, sr = cos_s[...], sin_s[...]
        cos_s[...] = cr * cb - sr * sb
        sin_s[...] = sr * cb + cr * sb
    with jax.named_scope("bar"):
        pl.semaphore_wait(barrier, SP - 1)

    def turned(t):
        t = t.astype(BF16).astype(F32)
        return (t * cos_s[...] + pltpu.roll(t, HEAD // 2, 1) * sin_s[...]).astype(BF16)

    def project_kv(g, _):
        slot = g % 2
        with jax.named_scope("kvwait"):
            for c in w_kv(g, slot):
                c.wait()
        r = _dot(a_s[...], wkv_s[slot], 1, 0)
        kv[g, me, 0] = turned(r[:, :HEAD])
        vt = r[:, HEAD:].T.astype(BF16)
        for n in range(T // HEAD):
            kv[g, me, 1, n * HEAD : (n + 1) * HEAD, :] = vt[:, n * HEAD : (n + 1) * HEAD]

        @pl.when(g + 2 < kv_heads)
        def _():
            for c in w_kv(g + 2, slot):
                c.start()

        for p in range(2):

            @pl.when(g == 2 * p + 2)
            def _():
                for c in w_q(p, p):
                    c.start()

        sends_own(g, start)
        return 0

    with jax.named_scope("kvall"):
        lax.fori_loop(0, kv_heads, project_kv, 0)

    def project_q(p, _):
        slot = p % 2
        with jax.named_scope("qwait"):
            for c in w_q(p, slot):
                c.wait()
        r = _dot(a_s[...], w_s[slot, :D, :], 1, 0)
        for i in range(2 * group):
            xq_s[:, pl.ds(pl.multiple_of(p * pw + i * HEAD, HEAD), HEAD)] = turned(r[:, i * HEAD : (i + 1) * HEAD])

        @pl.when(p + 2 < pairs)
        def _():
            for c in w_q(p + 2, slot):
                c.start()

        @pl.when(p + 2 >= pairs)
        def _():
            for c in w_o(p + 2 - pairs, slot):
                c.start()

        for h in range(2):
            g = 2 * p + h

            @pl.when((chip == last) & is_back(g))
            def _():
                query_back(g).start()

        return 0

    with jax.named_scope("qall"):
        lax.fori_loop(0, pairs, project_q, 0)

    def clear():
        top_s[...] = jnp.full(top_s.shape, NEG, F32)
        mix_s[...] = jnp.zeros(mix_s.shape, F32)

    def block(q, g, srcs, diagonal=False):
        keys = [kv[g, src, 0] for src in srcs]
        keys = keys[0] if len(srcs) == 1 else jnp.concatenate(keys, axis=0)
        values = jnp.concatenate([kv[g, src, 1, n * HEAD : (n + 1) * HEAD, :] for src in srcs for n in range(T // HEAD)], axis=1)
        values = jnp.concatenate([values, jnp.ones((8, values.shape[1]), BF16)], axis=0)
        strip = min(STRIP, T)
        strips = [(i, slice(at, at + strip)) for i in range(group) for at in range(0, T, strip)]
        ends = [keys.shape[0] - (T - at.stop if diagonal else 0) for _, at in strips]
        scores = [_dot(keys[:end], q(i, at), 1, 1) for (i, at), end in zip(strips, ends)]
        weights, keeps = [], []
        for (i, at), end, s in zip(strips, ends, scores):
            if diagonal:
                place = lax.broadcasted_iota(jnp.int32, s.shape, 1) - lax.broadcasted_iota(jnp.int32, s.shape, 0)
                s = jnp.where(place >= strip - end, s, HIDDEN)
            top = s.max(axis=0, keepdims=True)
            if not diagonal:
                old = top_s[i : i + 1, at]
                top = jnp.maximum(old, top)
                keeps.append(jnp.exp2((old - top) * E))
            top_s[i : i + 1, at] = top
            weights.append(jnp.exp2((s - top) * E).astype(BF16))
        for n, ((i, at), end, p) in enumerate(zip(strips, ends, weights)):
            mix = _dot(values[:, :end], p, 1, 0)
            mix_s[i, :, at] = mix if diagonal else mix_s[i, :, at] * keeps[n] + mix

    def pass_on(g, e):
        src = e * CORES + core
        with jax.named_scope("gotremote"):
            got(g, src)
        sends_on(g, src, start)

    def attend(t, _):
        g = head_of(t)
        p, slot = t // 2, (t // 2) % 2
        back = is_back(g)
        remotes = jnp.where((chip == last) & back, 0, chip)

        def own_q(i, at):
            return xq_s[at, pl.ds(pl.multiple_of(g * gw + i * HEAD, HEAD), HEAD)]

        @pl.when((chip == before) & (g + AHEAD < kv_heads))
        def _():
            for e in (1, 0):
                pass_on(g + AHEAD, e)

        @pl.when((chip == before) & back)
        def _():
            i3 = back_index(g)
            with jax.named_scope("gotq3"):
                query_back(g).wait_recv()
            got(g, other)
            for e in range(before):
                got(g, e * CORES + 1 - core)
            clear()

            def remote3(e, _):
                with jax.named_scope("block3"):
                    block(lambda i, at: q3[i3, at, i * HEAD : (i + 1) * HEAD], g, (CORES * e, CORES * e + 1))
                return 0

            lax.fori_loop(0, last, remote3, 0)
            st3[i3, 0:8, :] = top_s[...]
            for i in range(group):
                total = mix_s[i, HEAD : HEAD + 1, :]
                st3[i3, 8 + i : 9 + i, :] = total
                o3[i3, i] = (mix_s[i, :HEAD, :] * (1 / total)).astype(BF16)
            for c in result_back(i3, me + CORES):
                c.start()

        @pl.when((chip != before) & (remotes > 0))
        def _():
            pass_on(g, chip - 1)

        with jax.named_scope("diag"):

            @pl.when(core == 0)
            def _():
                block(own_q, g, (me,), True)

            @pl.when(jnp.logical_not((chip == before) & back))
            def _():
                got(g, other)

            @pl.when(core == 1)
            def _():
                block(own_q, g, (other, me), True)

        def remote(j, _):
            e = chip - 1 - j
            late = t == kv_heads - 1

            @pl.when((chip != before) & (e > 0) & jnp.logical_not(late))
            def _():
                pass_on(g, e - 1)

            @pl.when(jnp.logical_not((chip == before) & back))
            def _():
                with jax.named_scope("gotother"):
                    got(g, e * CORES + 1 - core)

            with jax.named_scope("block"):
                block(own_q, g, (CORES * e, CORES * e + 1))

            @pl.when((chip != before) & (e > 0) & late)
            def _():
                pass_on(g, e - 1)

            return 0

        lax.fori_loop(0, remotes, remote, 0)

        @pl.when((chip == last) & back)
        def _():
            i3 = back_index(g)
            with jax.named_scope("gotback"):
                for c in result_back(i3, me - CORES):
                    c.wait_recv()
            for i in range(group):
                mine, theirs = top_s[i : i + 1, :], st3[i3, i : i + 1, :]
                top = jnp.maximum(mine, theirs)
                a = jnp.exp2((mine - top) * E)
                b = jnp.exp2((theirs - top) * E) * st3[i3, 8 + i : 9 + i, :]
                mix_s[i, :HEAD, :] = mix_s[i, :HEAD, :] * a + o3[i3, i].astype(F32) * b
                mix_s[i, HEAD:, :] = mix_s[i, HEAD:, :] * a + b

        for i in range(group):
            total = mix_s[i, HEAD : HEAD + 1, :]
            at = pl.ds(pl.multiple_of(t % 2 * gw + i * HEAD, HEAD), HEAD)
            o_s[:, at] = (mix_s[i, :HEAD, :] * (1 / total)).T.astype(BF16)

        def project(first, heads, out_ref):
            rows = slice(first * gw, (first + heads) * gw)
            for n in range(4):
                at = slice(n * wide, (n + 1) * wide)
                y = y_s[:, at] + _dot(o_s[:, rows], w_s[slot, n * pw + rows.start : n * pw + rows.stop, :wide], 1, 0)
                out_ref[:, at] = y.astype(out_ref.dtype)

        @pl.when((t % 2 == 1) & (t < kv_heads - 1))
        def _():
            with jax.named_scope("oproj"):
                for c in w_o(p, slot):
                    c.wait()
                project(0, 2, y_s)

            @pl.when(p + 2 < pairs)
            def _():
                for c in w_o(p + 2, slot):
                    c.start()

        @pl.when(t == kv_heads - 2)
        def _():
            for c in w_o(p, slot):
                c.wait()
            project(0, 1, y_s)

        @pl.when(t == kv_heads - 1)
        def _():
            with jax.named_scope("olast"):
                project(1, 1, y_ref)

        return 0

    @pl.when(chip == before)
    def _():
        for g in range(AHEAD):
            for e in (1, 0):
                pass_on(g, e)

    lax.fori_loop(0, kv_heads, attend, 0)

    def drain(g, _):
        sends_own(g, finish)

        def on(e, _):
            sends_on(g, e * CORES + core, finish)
            return 0

        lax.fori_loop(0, jnp.where((chip == last) & is_back(g), 0, chip), on, 0)

        @pl.when((chip == last) & is_back(g))
        def _():
            query_back(g).wait_send()

        @pl.when((chip == before) & is_back(g))
        def _():
            for c in result_back(back_index(g), me + CORES):
                c.wait_send()

        return 0

    with jax.named_scope("drain"):
        lax.fori_loop(0, kv_heads, drain, 0)


def rope_tables(T):
    half = HEAD // 2
    rate = float(THETA) ** (-np.arange(half) / half)
    sign = np.concatenate([-np.ones(half), np.ones(half)])

    def table(place):
        angle = np.tile(place[:, None] * rate, (1, 2))
        return np.cos(angle).astype(np.float32), (np.sin(angle) * sign).astype(np.float32)

    return np.concatenate(table(np.arange(SP) * T)), *table(np.arange(T))


def layer(x, gain, wq, wk, wv, wo):
    T, D = x.shape
    kv_heads = wk.shape[1] // HEAD
    group = wq.shape[1] // wk.shape[1]
    gw = group * HEAD
    pw = 2 * gw
    nb = len(BACK)
    dma = pltpu.SemaphoreType.DMA
    hbm, vmem = pl.BlockSpec(memory_space=pl.ANY), pl.BlockSpec(memory_space=pltpu.VMEM)
    flops = 2 * T * D * (2 * wq.shape[1] + 2 * wk.shape[1]) + 4 * T * T * SP * wq.shape[1] // 2
    return pl.pallas_call(
        functools.partial(_kernel, kv_heads=kv_heads, group=group),
        out_shape=pltpu.VMEM((T, D), BF16),
        in_specs=[hbm, vmem, vmem, hbm, hbm, hbm, hbm, hbm, hbm],
        out_specs=vmem,
        scratch_shapes=[
            pltpu.VMEM((T, D), BF16),
            pltpu.VMEM((T, D), BF16),
            pltpu.VMEM((1, D), F32),
            pltpu.VMEM((T, HEAD), F32),
            pltpu.VMEM((T, HEAD), F32),
            pltpu.VMEM((2, D, 2 * HEAD), BF16),
            pltpu.VMEM((2, max(D, 4 * pw), max(pw, D // 4)), BF16),
            pltpu.VMEM((kv_heads, SP, 2, T, HEAD), BF16),
            pltpu.VMEM((nb, T, gw), BF16),
            pltpu.VMEM((nb, group, HEAD, T), BF16),
            pltpu.VMEM((nb, 16, T), F32),
            pltpu.VMEM((T, D), F32),
            pltpu.VMEM((T, pw), BF16),
            pltpu.VMEM((8, T), F32),
            pltpu.VMEM((group, HEAD + 8, T), F32),
            dma((4,)), dma((2,)), dma((2, 2)), dma((2, 8)),
            dma((3, kv_heads, SP)), dma((kv_heads, SP)), dma((nb,)), dma((nb,)), dma((2, nb)), dma((2, nb)),
        ],
        compiler_params=pltpu.CompilerParams(collective_id=0, has_side_effects=True, vmem_limit_bytes=VMEM),
        cost_estimate=pl.CostEstimate(flops=flops, transcendentals=T * T * SP * wq.shape[1] // HEAD, bytes_accessed=60 * 2**20),
    )(x, gain.reshape(D // HEAD, HEAD), *rope_tables(T), wq, wk, wv, wo)


def solution(mesh):
    tokens, whole = P(("dp", "sp"), None), P(None, None)
    return jax.shard_map(
        layer,
        mesh=mesh,
        in_specs=(tokens, P(None), whole, whole, whole, whole),
        out_specs=tokens,
        check_vma=False,
    )
```

```python
import functools

import jax
import jax.numpy as jnp
import numpy as np
from jax import lax
from jax.experimental import pallas as pl
from jax.experimental.pallas import tpu as pltpu
from jax.sharding import PartitionSpec as P

HEAD = 128
THETA = 10000
NEG = -1e30
HIDDEN = 2 * NEG
LOG2E = 1.4426950408889634
E = HEAD**-0.5 * LOG2E
VMEM = 60 * 2**20
BACK = (1, 3, 5, 7)
ORDER = (0, 1, 2, 3, 4, 5, 6, 7)
CHIPS = 4
CORES = 2
SP = CHIPS * CORES
F32, BF16 = jnp.float32, jnp.bfloat16


def _dot(a, b, ca, cb):
    return lax.dot_general(a, b, (((ca,), (cb,)), ((), ())), preferred_element_type=F32)


def _kernel(x_ref, gain_ref, base_ref, cos_ref, sin_ref, wq_ref, wk_ref, wv_ref, wo_ref, y_ref,
            xq_s, a_s, gain_s, cos_s, sin_s, wkv_s, w_s, kv, o3, st3, y_s, o_s, top_s, mix_s, even_s, odd_s,
            x_sem, rope_sem, wkv_sem, w_sem, send_sem, recv_sem, qsend_sem, qrecv_sem, osend_sem, orecv_sem,
            *, kv_heads, group):
    T, D = x_ref.shape
    gw = group * HEAD
    pw = 2 * gw
    pairs = kv_heads // 2
    me = lax.axis_index("sp")
    chip, core = me // CORES, me % CORES
    other = me + 1 - 2 * core
    last, before = CHIPS - 1, CHIPS - 2

    def is_back(g):
        found = g == BACK[0]
        for b in BACK[1:]:
            found = found | (g == b)
        return found

    def back_index(g):
        return sum((g > b).astype(jnp.int32) for b in BACK)

    parts = 4
    rows = T // parts

    def x_part(i):
        at = pl.ds(i * rows, rows)
        return pltpu.make_async_copy(x_ref.at[at, :], xq_s.at[at, pl.ds(0, D)], x_sem.at[i])

    def ropes():
        return (pltpu.make_async_copy(cos_ref, cos_s, rope_sem.at[0]), pltpu.make_async_copy(sin_ref, sin_s, rope_sem.at[1]))

    def w_kv(g, slot):
        at = pl.ds(pl.multiple_of(g * HEAD, HEAD), HEAD)
        return (pltpu.make_async_copy(wk_ref.at[:, at], wkv_s.at[slot, :, pl.ds(0, HEAD)], wkv_sem.at[slot, 0]),
                pltpu.make_async_copy(wv_ref.at[:, at], wkv_s.at[slot, :, pl.ds(HEAD, HEAD)], wkv_sem.at[slot, 1]))

    def w_q(p, slot):
        return [w_q_part(p, slot, n) for n in range(4)]

    def w_q_part(p, slot, n):
        at = pl.ds(pl.multiple_of(n * (D // 4), HEAD), D // 4)
        return pltpu.make_async_copy(wq_ref.at[at, pl.ds(pl.multiple_of(p * pw, HEAD), pw)], w_s.at[slot, at, pl.ds(0, pw)],
                                     w_sem.at[slot, n])

    wide = D // 4

    def head_of(t):
        mine = sum(jnp.where(t == n, g, 0) for n, g in enumerate(ORDER))
        return jnp.where(chip == last, mine, t)

    def w_o(p, slot):
        at = [pl.ds(pl.multiple_of(head_of(2 * p + h) * gw, HEAD), gw) for h in range(2)]
        return [pltpu.make_async_copy(wo_ref.at[at[h], pl.ds(n * wide, wide)],
                                      w_s.at[slot, pl.ds(n * pw + h * gw, gw), pl.ds(0, wide)], w_sem.at[slot, 4 * h + n])
                for h in range(2) for n in range(4)]

    def piece(g, src, kind, target):
        return pltpu.make_async_remote_copy(src_ref=kv.at[g, src], dst_ref=kv.at[g, src], send_sem=send_sem.at[kind, g, src],
                                            recv_sem=recv_sem.at[g, src], device_id={"sp": target})

    def got(g, src):
        piece(g, src, 0, other).wait_recv()

    def q_at(g):
        return pl.ds(pl.multiple_of(g * gw, HEAD), gw)

    def query_back(g):
        i = back_index(g)
        return pltpu.make_async_remote_copy(src_ref=xq_s.at[:, q_at(g)], dst_ref=xq_s.at[:, q_at(kv_heads + i)], send_sem=qsend_sem.at[i],
                                            recv_sem=qrecv_sem.at[i], device_id={"sp": me - CORES})

    def result_back(i, target):
        return (pltpu.make_async_remote_copy(src_ref=o3.at[i], dst_ref=o3.at[i], send_sem=osend_sem.at[0, i],
                                             recv_sem=orecv_sem.at[0, i], device_id={"sp": target}),
                pltpu.make_async_remote_copy(src_ref=st3.at[i], dst_ref=st3.at[i], send_sem=osend_sem.at[1, i],
                                             recv_sem=orecv_sem.at[1, i], device_id={"sp": target}))

    def sends_own(g, do):
        do(lambda: piece(g, me, 0, other), None)
        do(lambda: piece(g, me, 1, me + CORES), (chip < before) | ((chip == before) & jnp.logical_not(is_back(g))))
        do(lambda: piece(g, me, 2, me + 2 * CORES), chip == 0)

    def sends_on(g, src, do):
        do(lambda: piece(g, src, 0, other), None)
        do(lambda: piece(g, src, 1, me + CORES), (chip == before) & jnp.logical_not(is_back(g)))

    def start(copy, cond):
        if cond is None:
            copy().start()
        else:
            pl.when(cond)(lambda: copy().start())

    def finish(copy, cond):
        if cond is None:
            copy().wait_send()
        else:
            pl.when(cond)(lambda: copy().wait_send())

    for i in range(parts):
        x_part(i).start()
    barrier = pltpu.get_barrier_semaphore()
    for d in range(1, SP):
        pl.semaphore_signal(barrier, inc=1, device_id={"sp": lax.rem(me + d, SP)})
    for c in (*w_kv(0, 0), *ropes(), *w_kv(1, 1)):
        c.start()
    for n in range(D // HEAD):
        gain_s[:, n * HEAD : (n + 1) * HEAD] = gain_ref[n : n + 1, :].astype(F32)
    for i in range(parts):
        with jax.named_scope("waitx"):
            x_part(i).wait()
        step = min(rows, 64)
        for at in range(i * rows, (i + 1) * rows, step):
            x = xq_s[at : at + step, :D].astype(F32)
            scale = lax.rsqrt(jnp.mean(x * x, -1, keepdims=True) + 1e-6)
            a_s[at : at + step, :] = (x * scale * gain_s[...]).astype(BF16)
            y_s[at : at + step, :] = x
    with jax.named_scope("rope"):
        for c in ropes():
            c.wait()
        cb, sb = base_ref[pl.ds(me, 1), :], base_ref[pl.ds(SP + me, 1), :]
        cr, sr = cos_s[...], sin_s[...]
        cos_s[...] = cr * cb - sr * sb
        sin_s[...] = sr * cb + cr * sb
    with jax.named_scope("bar"):
        pl.semaphore_wait(barrier, SP - 1)

    def turned(t):
        t = t.astype(BF16).astype(F32)
        return (t * cos_s[...] + pltpu.roll(t, HEAD // 2, 1) * sin_s[...]).astype(BF16)

    def project_kv(g, _):
        slot = g % 2
        with jax.named_scope("kvwait"):
            for c in w_kv(g, slot):
                c.wait()
        r = _dot(a_s[...], wkv_s[slot], 1, 0)
        kv[g, me, 0] = turned(r[:, :HEAD])
        vt = r[:, HEAD:].T.astype(BF16)
        for n in range(T // HEAD):
            kv[g, me, 1, n * HEAD : (n + 1) * HEAD, :] = vt[:, n * HEAD : (n + 1) * HEAD]

        @pl.when(g + 2 < kv_heads)
        def _():
            for c in w_kv(g + 2, slot):
                c.start()

        @pl.when(g < 8)
        def _():
            w_q_part(g // 4, g // 4, g % 4).start()

        sends_own(g, start)
        return 0

    with jax.named_scope("kvall"):
        lax.fori_loop(0, kv_heads, project_kv, 0)

    def pass_on(g, e):
        src = e * CORES + core
        with jax.named_scope("gotremote"):
            got(g, src)
        sends_on(g, src, start)

    def project_q(p, _):
        slot = p % 2
        with jax.named_scope("qwait"):
            for c in w_q(p, slot):
                c.wait()
        r = _dot(a_s[...], w_s[slot, :D, :pw], 1, 0)
        for i in range(2 * group):
            xq_s[:, pl.ds(pl.multiple_of(p * pw + i * HEAD, HEAD), HEAD)] = turned(r[:, i * HEAD : (i + 1) * HEAD])

        @pl.when(p + 2 < pairs)
        def _():
            for c in w_q(p + 2, slot):
                c.start()

        @pl.when(p + 2 >= pairs)
        def _():
            for c in w_o(p + 2 - pairs, slot):
                c.start()

        for h in range(2):
            g = 2 * p + h

            @pl.when((chip == last) & is_back(g))
            def _():
                query_back(g).start()

        return 0

    with jax.named_scope("qall"):
        lax.fori_loop(0, pairs, project_q, 0)

    def half(now, nxt, state, g, src, then, first=False, diagonal=False):
        qc, g_then, src_then = then
        keys = kv[g_then, src_then, 0]
        values = jnp.concatenate([kv[g, src, 1, n * HEAD : (n + 1) * HEAD, :] for n in range(T // HEAD)], axis=1)
        values = jnp.concatenate([values, jnp.ones((8, T), BF16)], axis=0)
        strip = T // 2 if diagonal and T > HEAD else T
        for i in range(group):
            q = xq_s[:, pl.ds(pl.multiple_of(qc + i * HEAD, HEAD), HEAD)]
            for a in range(0, T, strip):
                at = slice(a, a + strip)
                nxt[i, :, at] = _dot(keys, q[at], 1, 1)
                end = a + strip if diagonal else T
                s = now[i, :end, at]
                if diagonal:
                    place = lax.broadcasted_iota(jnp.int32, s.shape, 1) - lax.broadcasted_iota(jnp.int32, s.shape, 0)
                    s = jnp.where(place >= -a, s, HIDDEN)
                top = s.max(axis=0, keepdims=True)
                if first:
                    top_s[state, i : i + 1, at] = top
                    mix_s[state, i, :, at] = _dot(values[:, :end], jnp.exp2((s - top) * E).astype(BF16), 1, 0)
                else:
                    old = top_s[state, i : i + 1, at]
                    top = jnp.maximum(old, top)
                    top_s[state, i : i + 1, at] = top
                    mix = _dot(values[:, :end], jnp.exp2((s - top) * E).astype(BF16), 1, 0)
                    mix_s[state, i, :, at] = mix_s[state, i, :, at] * jnp.exp2((old - top) * E) + mix

    def either(cond, a, b):
        return tuple(jnp.where(cond, x, y) for x, y in zip(a, b))

    def unit(state, g, qc, e, then):
        half(even_s, odd_s, state, g, e * CORES + core, (qc, g, e * CORES + 1 - core))
        half(odd_s, even_s, state, g, e * CORES + 1 - core, then)

    def is_guest(t):
        return (chip == before) & is_back(head_of(t)) & (t >= 0) & (t < kv_heads)

    def own_units(t):
        n = jnp.where((chip == last) & is_back(head_of(t)), 0, jnp.minimum(chip, last - 1))
        return jnp.where((t >= 0) & (t < kv_heads), n, 0)

    def units(t):
        return jnp.where(is_guest(t), 5, own_units(t))

    def unit_chip(t, k):
        return jnp.where(is_guest(t), last - 1 - (k + 1) // 2, own_units(t) - 1 - k)

    def for_guest(t, k):
        return is_guest(t) & ((k < 2) | (k == 3))

    def arriving(t, k):
        return jnp.logical_not(is_guest(t)) | (k == 1) | (k == 3)

    def column(t, k):
        g = head_of(t)
        return jnp.where(for_guest(t, k), kv_heads + back_index(g), g) * gw

    def item_diagonal(t):
        g = head_of(t)
        return g * gw, g, jnp.where(core == 1, other, me)

    def item_unit(t, k):
        return column(t, k), head_of(t), unit_chip(t, k) * CORES + core

    nothing = (jnp.int32(0), jnp.int32(0), me)

    def item_first(t):
        return either(t < kv_heads - 1, item_diagonal(t + 1), either(units(t) > 0, item_unit(t, 0), nothing))

    def enter_diagonal(t):
        with jax.named_scope("gotown"):
            got(head_of(t), other)

    def enter_unit(t, k):
        @pl.when(is_guest(t) & (k == 0))
        def _():
            with jax.named_scope("gotq3"):
                query_back(head_of(t)).wait_recv()

        @pl.when(arriving(t, k))
        def _():
            pass_on(head_of(t), unit_chip(t, k))

    def enter_first(t):
        @pl.when(t < kv_heads - 1)
        def _():
            enter_diagonal(t + 1)

        @pl.when((t == kv_heads - 1) & (units(t) > 0))
        def _():
            enter_unit(t, 0)

    def enter_after_diagonal(t):
        @pl.when(units(t) > 0)
        def _():
            enter_unit(t, 0)

        @pl.when(units(t) == 0)
        def _():
            enter_first(t + 1)

    def attend(t, _):
        g = head_of(jnp.maximum(t, 0))
        p, slot, state = t // 2, (t // 2) % 2, t % 2
        back = is_back(g)
        i3 = back_index(g)
        n = units(t)
        after_diagonal = either(n > 0, item_unit(t, 0), item_first(t + 1))

        @pl.when(t + 1 < kv_heads)
        def _():
            g1 = head_of(t + 1)
            state1 = (t + 1) % 2
            near = (chip == last) & jnp.logical_not(is_back(g1))
            then = either(near, (g1 * gw, g1, (last - 1) * CORES + core), after_diagonal)

            @pl.when(near)
            def _():
                pass_on(g1, last - 1)

            @pl.when(jnp.logical_not(near))
            def _():
                enter_after_diagonal(t)

            @pl.when(core == 1)
            def _():
                with jax.named_scope("diag1"):
                    half(even_s, odd_s, state1, g1, other, (g1 * gw, g1, me), first=True)
                    half(odd_s, even_s, state1, g1, me, then, diagonal=True)

            @pl.when(core == 0)
            def _():
                with jax.named_scope("diag0"):
                    scores(item_diagonal(t + 1), odd_s)
                    half(odd_s, even_s, state1, g1, me, then, first=True, diagonal=True)

            @pl.when(near)
            def _():
                with jax.named_scope("gotother"):
                    got(g1, (last - 1) * CORES + 1 - core)
                enter_after_diagonal(t)
                with jax.named_scope("near"):
                    unit(state1, g1, g1 * gw, last - 1, after_diagonal)

        @pl.when(is_guest(t))
        def _():
            top_s[2] = jnp.full(top_s.shape[1:], NEG, F32)
            mix_s[2] = jnp.zeros(mix_s.shape[1:], F32)

        def rest(k, _):
            e = unit_chip(t, k)

            @pl.when(arriving(t, k))
            def _():
                with jax.named_scope("gotother"):
                    got(g, e * CORES + 1 - core)

            @pl.when(k + 1 < n)
            def _():
                enter_unit(t, k + 1)

            @pl.when(k + 1 == n)
            def _():
                enter_first(t + 1)

            with jax.named_scope("rest"):
                unit(jnp.where(for_guest(t, k), 2, state), g, column(t, k), e, either(k + 1 < n, item_unit(t, k + 1), item_first(t + 1)))

            @pl.when(is_guest(t) & (k == 3))
            def _():
                st3[i3, 0:8, :] = top_s[2]
                for i in range(group):
                    total = mix_s[2, i, HEAD : HEAD + 1, :]
                    st3[i3, 8 + i : 9 + i, :] = total
                    o3[i3, i] = (mix_s[2, i, :HEAD, :] * (1 / total)).astype(BF16)
                for c in result_back(i3, me + CORES):
                    c.start()

            return 0

        lax.fori_loop(0, n, rest, 0)

        @pl.when(t >= 0)
        def _():
            complete(t, g, p, slot, state, back)

        return 0

    def scores(item, to):
        qc, g, src = item
        for i in range(group):
            to[i] = _dot(kv[g, src, 0], xq_s[:, pl.ds(pl.multiple_of(qc + i * HEAD, HEAD), HEAD)], 1, 1)

    def complete(t, g, p, slot, state, back):
        @pl.when((chip == last) & back)
        def _():
            i3 = back_index(g)
            with jax.named_scope("gotback"):
                for c in result_back(i3, me - CORES):
                    c.wait_recv()
            for i in range(group):
                mine, theirs = top_s[state, i : i + 1, :], st3[i3, i : i + 1, :]
                top = jnp.maximum(mine, theirs)
                a = jnp.exp2((mine - top) * E)
                b = jnp.exp2((theirs - top) * E) * st3[i3, 8 + i : 9 + i, :]
                mix_s[state, i, :HEAD, :] = mix_s[state, i, :HEAD, :] * a + o3[i3, i].astype(F32) * b
                mix_s[state, i, HEAD:, :] = mix_s[state, i, HEAD:, :] * a + b

        for i in range(group):
            total = mix_s[state, i, HEAD : HEAD + 1, :]
            at = pl.ds(pl.multiple_of(t % 2 * gw + i * HEAD, HEAD), HEAD)
            o_s[:, at] = (mix_s[state, i, :HEAD, :] * (1 / total)).T.astype(BF16)

        def project(first, heads, out_ref):
            rows = slice(first * gw, (first + heads) * gw)
            for n in range(4):
                at = slice(n * wide, (n + 1) * wide)
                y = y_s[:, at] + _dot(o_s[:, rows], w_s[slot, n * pw + rows.start : n * pw + rows.stop, :wide], 1, 0)
                out_ref[:, at] = y.astype(out_ref.dtype)

        @pl.when((t % 2 == 1) & (t < kv_heads - 1))
        def _():
            with jax.named_scope("oproj"):
                for c in w_o(p, slot):
                    c.wait()
                project(0, 2, y_s)

            @pl.when(p + 2 < pairs)
            def _():
                for c in w_o(p + 2, slot):
                    c.start()

        @pl.when(t == kv_heads - 2)
        def _():
            for c in w_o(p, slot):
                c.wait()
            project(0, 1, y_s)

        @pl.when(t == kv_heads - 1)
        def _():
            with jax.named_scope("olast"):
                project(1, 1, y_ref)

    enter_diagonal(0)
    scores(item_diagonal(0), even_s)
    lax.fori_loop(-1, kv_heads, attend, 0)

    def drain(g, _):
        sends_own(g, finish)

        def on(e, _):
            sends_on(g, e * CORES + core, finish)
            return 0

        lax.fori_loop(0, jnp.where((chip == last) & is_back(g), 0, chip), on, 0)

        @pl.when((chip == last) & is_back(g))
        def _():
            query_back(g).wait_send()

        @pl.when((chip == before) & is_back(g))
        def _():
            for c in result_back(back_index(g), me + CORES):
                c.wait_send()

        return 0

    with jax.named_scope("drain"):
        lax.fori_loop(0, kv_heads, drain, 0)


def rope_tables(T):
    half = HEAD // 2
    rate = float(THETA) ** (-np.arange(half) / half)
    sign = np.concatenate([-np.ones(half), np.ones(half)])

    def table(place):
        angle = np.tile(place[:, None] * rate, (1, 2))
        return np.cos(angle).astype(np.float32), (np.sin(angle) * sign).astype(np.float32)

    return np.concatenate(table(np.arange(SP) * T)), *table(np.arange(T))


def layer(x, gain, wq, wk, wv, wo):
    T, D = x.shape
    kv_heads = wk.shape[1] // HEAD
    group = wq.shape[1] // wk.shape[1]
    gw = group * HEAD
    pw = 2 * gw
    nb = len(BACK)
    dma = pltpu.SemaphoreType.DMA
    hbm, vmem = pl.BlockSpec(memory_space=pl.ANY), pl.BlockSpec(memory_space=pltpu.VMEM)
    flops = 2 * T * D * (2 * wq.shape[1] + 2 * wk.shape[1]) + 4 * T * T * SP * wq.shape[1] // 2
    return pl.pallas_call(
        functools.partial(_kernel, kv_heads=kv_heads, group=group),
        out_shape=pltpu.VMEM((T, D), BF16),
        in_specs=[hbm, vmem, vmem, hbm, hbm, hbm, hbm, hbm, hbm],
        out_specs=vmem,
        scratch_shapes=[
            pltpu.VMEM((T, max(D, (kv_heads + nb) * gw)), BF16),
            pltpu.VMEM((T, D), BF16),
            pltpu.VMEM((1, D), F32),
            pltpu.VMEM((T, HEAD), F32),
            pltpu.VMEM((T, HEAD), F32),
            pltpu.VMEM((2, D, 2 * HEAD), BF16),
            pltpu.VMEM((2, max(D, 4 * pw), max(pw, D // 4)), BF16),
            pltpu.VMEM((kv_heads, SP, 2, T, HEAD), BF16),
            pltpu.VMEM((nb, group, HEAD, T), BF16),
            pltpu.VMEM((nb, 16, T), F32),
            pltpu.VMEM((T, D), F32),
            pltpu.VMEM((T, pw), BF16),
            pltpu.VMEM((3, 8, T), F32),
            pltpu.VMEM((3, group, HEAD + 8, T), F32),
            pltpu.VMEM((group, T, T), F32),
            pltpu.VMEM((group, T, T), F32),
            dma((4,)), dma((2,)), dma((2, 2)), dma((2, 8)),
            dma((3, kv_heads, SP)), dma((kv_heads, SP)), dma((nb,)), dma((nb,)), dma((2, nb)), dma((2, nb)),
        ],
        compiler_params=pltpu.CompilerParams(collective_id=0, has_side_effects=True, vmem_limit_bytes=VMEM),
        cost_estimate=pl.CostEstimate(flops=flops, transcendentals=T * T * SP * wq.shape[1] // HEAD, bytes_accessed=60 * 2**20),
    )(x, gain.reshape(D // HEAD, HEAD), *rope_tables(T), wq, wk, wv, wo)


def solution(mesh):
    tokens, whole = P(("dp", "sp"), None), P(None, None)
    return jax.shard_map(
        layer,
        mesh=mesh,
        in_specs=(tokens, P(None), whole, whole, whole, whole),
        out_specs=tokens,
        check_vma=False,
    )
```

```python
import functools

import jax
import jax.numpy as jnp
import numpy as np
from jax import lax
from jax.experimental import pallas as pl
from jax.experimental.pallas import tpu as pltpu
from jax.sharding import PartitionSpec as P

HEAD = 128
THETA = 10000
NEG = -1e30
HIDDEN = 2 * NEG
LOG2E = 1.4426950408889634
E = HEAD**-0.5 * LOG2E
VMEM = 60 * 2**20
BACK = (1, 3, 5, 7)
ORDER = (0, 1, 2, 3, 4, 5, 6, 7)
CHIPS = 4
CORES = 2
SP = CHIPS * CORES
F32, BF16 = jnp.float32, jnp.bfloat16


def _dot(a, b, ca, cb):
    return lax.dot_general(a, b, (((ca,), (cb,)), ((), ())), preferred_element_type=F32)


def _kernel(x_ref, gain_ref, base_ref, cos_ref, sin_ref, wq_ref, wk_ref, wv_ref, wo_ref, y_ref,
            xq_s, a_s, gain_s, cos_s, sin_s, wkv_s, w_s, kv, o3, st3, y_s, o_s, top_s, mix_s, even_s, odd_s,
            x_sem, rope_sem, wkv_sem, w_sem, send_sem, recv_sem, qsend_sem, qrecv_sem, osend_sem, orecv_sem,
            *, kv_heads, group):
    T, D = x_ref.shape
    gw = group * HEAD
    pw = 2 * gw
    pairs = kv_heads // 2
    me = lax.axis_index("sp")
    chip, core = me // CORES, me % CORES
    other = me + 1 - 2 * core
    last, before = CHIPS - 1, CHIPS - 2

    def is_back(g):
        found = g == BACK[0]
        for b in BACK[1:]:
            found = found | (g == b)
        return found

    def back_index(g):
        return sum((g > b).astype(jnp.int32) for b in BACK)

    parts = 4
    rows = T // parts

    def x_part(i):
        at = pl.ds(i * rows, rows)
        return pltpu.make_async_copy(x_ref.at[at, :], xq_s.at[at, pl.ds(0, D)], x_sem.at[i])

    def ropes():
        return (pltpu.make_async_copy(cos_ref, cos_s, rope_sem.at[0]), pltpu.make_async_copy(sin_ref, sin_s, rope_sem.at[1]))

    def w_kv(g, slot):
        at = pl.ds(pl.multiple_of(g * HEAD, HEAD), HEAD)
        return (pltpu.make_async_copy(wk_ref.at[:, at], wkv_s.at[slot, :, pl.ds(0, HEAD)], wkv_sem.at[slot, 0]),
                pltpu.make_async_copy(wv_ref.at[:, at], wkv_s.at[slot, :, pl.ds(HEAD, HEAD)], wkv_sem.at[slot, 1]))

    def w_q(p, slot):
        return [w_q_part(p, slot, n) for n in range(4)]

    def w_q_part(p, slot, n):
        at = pl.ds(pl.multiple_of(n * (D // 4), HEAD), D // 4)
        return pltpu.make_async_copy(wq_ref.at[at, pl.ds(pl.multiple_of(p * pw, HEAD), pw)], w_s.at[slot, at, pl.ds(0, pw)],
                                     w_sem.at[slot, n])

    wide = D // 4

    def head_of(t):
        mine = sum(jnp.where(t == n, g, 0) for n, g in enumerate(ORDER))
        return jnp.where(chip == last, mine, t)

    def w_o(p, slot):
        at = [pl.ds(pl.multiple_of(head_of(2 * p + h) * gw, HEAD), gw) for h in range(2)]
        return [pltpu.make_async_copy(wo_ref.at[at[h], pl.ds(n * wide, wide)],
                                      w_s.at[slot, pl.ds(n * pw + h * gw, gw), pl.ds(0, wide)], w_sem.at[slot, 4 * h + n])
                for h in range(2) for n in range(4)]

    def piece(g, src, kind, target):
        return pltpu.make_async_remote_copy(src_ref=kv.at[g, src], dst_ref=kv.at[g, src], send_sem=send_sem.at[kind, src // CORES],
                                            recv_sem=recv_sem.at[g, src], device_id={"sp": target})

    def got(g, src):
        piece(g, src, 0, other).wait_recv()

    def q_at(g):
        return pl.ds(pl.multiple_of(g * gw, HEAD), gw)

    def query_back(g):
        i = back_index(g)
        return pltpu.make_async_remote_copy(src_ref=xq_s.at[:, q_at(g)], dst_ref=xq_s.at[:, q_at(kv_heads + i)], send_sem=qsend_sem.at[i],
                                            recv_sem=qrecv_sem.at[i], device_id={"sp": me - CORES})

    def result_back(i, target):
        return (pltpu.make_async_remote_copy(src_ref=o3.at[i], dst_ref=o3.at[i], send_sem=osend_sem.at[0, i],
                                             recv_sem=orecv_sem.at[0, i], device_id={"sp": target}),
                pltpu.make_async_remote_copy(src_ref=st3.at[i], dst_ref=st3.at[i], send_sem=osend_sem.at[1, i],
                                             recv_sem=orecv_sem.at[1, i], device_id={"sp": target}))

    def send_own(g):
        piece(g, me, 0, other).start()

        @pl.when((chip < before) | ((chip == before) & jnp.logical_not(is_back(g))))
        def _():
            piece(g, me, 1, me + CORES).start()

        @pl.when(chip == 0)
        def _():
            piece(g, me, 2, me + 2 * CORES).start()

    def send_on(g, src):
        piece(g, src, 0, other).start()

        @pl.when((chip == before) & jnp.logical_not(is_back(g)))
        def _():
            piece(g, src, 1, me + CORES).start()

    def sent(kind, src, heads):
        at = pl.ds(0, heads)
        pltpu.make_async_remote_copy(src_ref=kv.at[at, src], dst_ref=kv.at[at, src], send_sem=send_sem.at[kind, src // CORES],
                                     recv_sem=recv_sem.at[0, src], device_id={"sp": other}).wait_send()

    half_t = T // 2
    place = lax.broadcasted_iota(jnp.int32, (half_t, half_t), 1) - lax.broadcasted_iota(jnp.int32, (half_t, half_t), 0)

    for i in range(parts):
        x_part(i).start()
    barrier = pltpu.get_barrier_semaphore()
    for d in range(1, SP):
        pl.semaphore_signal(barrier, inc=1, device_id={"sp": lax.rem(me + d, SP)})
    for c in (*w_kv(0, 0), *ropes(), *w_kv(1, 1)):
        c.start()
    for n in range(D // HEAD):
        gain_s[:, n * HEAD : (n + 1) * HEAD] = gain_ref[n : n + 1, :].astype(F32)
    for i in range(parts):
        with jax.named_scope("waitx"):
            x_part(i).wait()
        step = min(rows, 64)
        for at in range(i * rows, (i + 1) * rows, step):
            x = xq_s[at : at + step, :D].astype(F32)
            scale = lax.rsqrt(jnp.mean(x * x, -1, keepdims=True) + 1e-6)
            a_s[at : at + step, :] = (x * scale * gain_s[...]).astype(BF16)
    with jax.named_scope("rope"):
        for c in ropes():
            c.wait()
        cb, sb = base_ref[pl.ds(me, 1), :], base_ref[pl.ds(SP + me, 1), :]
        cr, sr = cos_s[...], sin_s[...]
        cos_s[...] = cr * cb - sr * sb
        sin_s[...] = sr * cb + cr * sb
    with jax.named_scope("bar"):
        pl.semaphore_wait(barrier, SP - 1)

    def turned(t):
        t = t.astype(BF16).astype(F32)
        return (t * cos_s[...] + pltpu.roll(t, HEAD // 2, 1) * sin_s[...]).astype(BF16)

    def project_kv(g, _):
        slot = g % 2
        with jax.named_scope("kvwait"):
            for c in w_kv(g, slot):
                c.wait()
        at = pl.ds(pl.multiple_of(g * (T // kv_heads), T // kv_heads), T // kv_heads)
        y_s[at, :] = xq_s[at, :D].astype(F32)
        r = _dot(a_s[...], wkv_s[slot], 1, 0)
        kv[g, me, 0] = turned(r[:, :HEAD])
        vt = r[:, HEAD:].T.astype(BF16)
        for n in range(T // HEAD):
            kv[g, me, 1, n * HEAD : (n + 1) * HEAD, :] = vt[:, n * HEAD : (n + 1) * HEAD]

        @pl.when(g + 2 < kv_heads)
        def _():
            for c in w_kv(g + 2, slot):
                c.start()

        @pl.when(g < 8)
        def _():
            w_q_part(g // 4, g // 4, g % 4).start()

        send_own(g)
        return 0

    with jax.named_scope("kvall"):
        lax.fori_loop(0, kv_heads, project_kv, 0)

    def pass_on(g, e):
        src = e * CORES + core
        with jax.named_scope("gotremote"):
            got(g, src)
        send_on(g, src)

    def project_q(p):
        slot = jnp.where(p == 1, 1, 0)
        with jax.named_scope("qwait"):
            for c in w_q(p, slot):
                c.wait()
        r = _dot(a_s[...], w_s[slot, :D, :pw], 1, 0)
        for i in range(2 * group):
            xq_s[:, pl.ds(pl.multiple_of(p * pw + i * HEAD, HEAD), HEAD)] = turned(r[:, i * HEAD : (i + 1) * HEAD])

        for done, copies in ((0, lambda: w_q(2, 0)), (1, lambda: w_o(0, 1)), (2, lambda: w_q(3, 0)), (3, lambda: w_o(2, 0))):

            @pl.when(p == done)
            def _():
                for c in copies():
                    c.start()

        for h in range(2):
            g = 2 * p + h

            @pl.when((chip == last) & is_back(g))
            def _():
                query_back(g).start()

    with jax.named_scope("q0"):
        project_q(jnp.int32(0))

    def half(now, nxt, state, g, src, then, first=False, diagonal=False):
        qc, g_then, src_then = then
        keys = kv[g_then, src_then, 0]
        values = jnp.concatenate([kv[g, src, 1, n * HEAD : (n + 1) * HEAD, :] for n in range(T // HEAD)], axis=1)
        values = jnp.concatenate([values, jnp.ones((8, T), BF16)], axis=0)
        strip = T // 2 if diagonal else T
        for i in range(group):
            q = xq_s[:, pl.ds(pl.multiple_of(qc + i * HEAD, HEAD), HEAD)]
            for a in range(0, T, strip):
                at = slice(a, a + strip)
                nxt[i, :, at] = _dot(keys, q[at], 1, 1)
                end = a + strip if diagonal else T
                s = now[i, :end, at]
                if diagonal:
                    cut = jnp.where(place >= 0, s[a:], HIDDEN)
                    s = jnp.concatenate([s[:a], cut], axis=0) if a else cut
                top = s.max(axis=0, keepdims=True)
                if first:
                    top_s[state, i : i + 1, at] = top
                    mix_s[state, i, :, at] = _dot(values[:, :end], jnp.exp2((s - top) * E).astype(BF16), 1, 0)
                else:
                    old = top_s[state, i : i + 1, at]
                    top = jnp.maximum(old, top)
                    top_s[state, i : i + 1, at] = top
                    mix = _dot(values[:, :end], jnp.exp2((s - top) * E).astype(BF16), 1, 0)
                    mix_s[state, i, :, at] = mix_s[state, i, :, at] * jnp.exp2((old - top) * E) + mix

    def either(cond, a, b):
        return tuple(jnp.where(cond, x, y) for x, y in zip(a, b))

    def unit(state, g, qc, e, then):
        half(even_s, odd_s, state, g, e * CORES + core, (qc, g, e * CORES + 1 - core))
        half(odd_s, even_s, state, g, e * CORES + 1 - core, then)

    def is_guest(t):
        return (chip == before) & is_back(head_of(t)) & (t >= 0) & (t < kv_heads)

    def own_units(t):
        n = jnp.where((chip == last) & is_back(head_of(t)), 0, jnp.minimum(chip, last - 1))
        return jnp.where((t >= 0) & (t < kv_heads), n, 0)

    def units(t):
        return jnp.where(is_guest(t), 5, own_units(t))

    def unit_chip(t, k):
        return jnp.where(is_guest(t), last - 1 - (k + 1) // 2, own_units(t) - 1 - k)

    def for_guest(t, k):
        return is_guest(t) & ((k < 2) | (k == 3))

    def arriving(t, k):
        return jnp.logical_not(is_guest(t)) | (k == 1) | (k == 3)

    def column(t, k):
        g = head_of(t)
        return jnp.where(for_guest(t, k), kv_heads + back_index(g), g) * gw

    def item_diagonal(t):
        g = head_of(t)
        return g * gw, g, jnp.where(core == 1, other, me)

    def item_unit(t, k):
        return column(t, k), head_of(t), unit_chip(t, k) * CORES + core

    nothing = (jnp.int32(0), jnp.int32(0), me)

    def item_first(t):
        return either(t < kv_heads - 1, item_diagonal(t + 1), either(units(t) > 0, item_unit(t, 0), nothing))

    def enter_diagonal(t):
        with jax.named_scope("gotown"):
            got(head_of(t), other)

    def enter_unit(t, k):
        @pl.when(is_guest(t) & (k == 0))
        def _():
            with jax.named_scope("gotq3"):
                query_back(head_of(t)).wait_recv()

        @pl.when(arriving(t, k))
        def _():
            pass_on(head_of(t), unit_chip(t, k))

    def enter_first(t):
        @pl.when(t < kv_heads - 1)
        def _():
            enter_diagonal(t + 1)

        @pl.when((t == kv_heads - 1) & (units(t) > 0))
        def _():
            enter_unit(t, 0)

    def enter_after_diagonal(t):
        @pl.when(units(t) > 0)
        def _():
            enter_unit(t, 0)

        @pl.when(units(t) == 0)
        def _():
            enter_first(t + 1)

    def attend(t, _):
        g = head_of(jnp.maximum(t, 0))
        p, state = t // 2, t % 2
        slot = jnp.where(p == 2, 0, 1)
        back = is_back(g)
        i3 = back_index(g)
        n = units(t)
        after_diagonal = either(n > 0, item_unit(t, 0), item_first(t + 1))

        @pl.when(t + 1 < kv_heads)
        def _():
            g1 = head_of(t + 1)
            state1 = (t + 1) % 2
            near = (chip == last) & jnp.logical_not(is_back(g1))
            then = either(near, (g1 * gw, g1, (last - 1) * CORES + core), after_diagonal)

            @pl.when(near)
            def _():
                pass_on(g1, last - 1)

            @pl.when(jnp.logical_not(near))
            def _():
                enter_after_diagonal(t)

            @pl.when(core == 1)
            def _():
                with jax.named_scope("diag1"):
                    half(even_s, odd_s, state1, g1, other, (g1 * gw, g1, me), first=True)
                    half(odd_s, even_s, state1, g1, me, then, diagonal=True)

            @pl.when(core == 0)
            def _():
                with jax.named_scope("diag0"):
                    scores(item_diagonal(t + 1), odd_s)
                    half(odd_s, even_s, state1, g1, me, then, first=True, diagonal=True)

            @pl.when(near)
            def _():
                with jax.named_scope("gotother"):
                    got(g1, (last - 1) * CORES + 1 - core)
                enter_after_diagonal(t)
                with jax.named_scope("near"):
                    unit(state1, g1, g1 * gw, last - 1, after_diagonal)

        @pl.when(is_guest(t))
        def _():
            top_s[2] = jnp.full(top_s.shape[1:], NEG, F32)
            mix_s[2] = jnp.zeros(mix_s.shape[1:], F32)

        def rest(k, _):
            e = unit_chip(t, k)

            @pl.when(arriving(t, k))
            def _():
                with jax.named_scope("gotother"):
                    got(g, e * CORES + 1 - core)

            @pl.when(k + 1 < n)
            def _():
                enter_unit(t, k + 1)

            @pl.when(k + 1 == n)
            def _():
                enter_first(t + 1)

            with jax.named_scope("rest"):
                unit(jnp.where(for_guest(t, k), 2, state), g, column(t, k), e, either(k + 1 < n, item_unit(t, k + 1), item_first(t + 1)))

            @pl.when(is_guest(t) & (k == 3))
            def _():
                st3[i3, 0:group, :] = top_s[2, 0:group, :]
                for i in range(group):
                    total = mix_s[2, i, HEAD : HEAD + 1, :]
                    st3[i3, group + i : group + i + 1, :] = total
                    o3[i3, i] = (mix_s[2, i, :HEAD, :] * (1 / total)).astype(BF16)
                for c in result_back(i3, me + CORES):
                    c.start()

            return 0

        lax.fori_loop(0, n, rest, 0)

        @pl.when(t >= 0)
        def _():
            complete(t, g, p, slot, state, back)

        @pl.when((t % 2 == 1) & (t < 4))
        def _():
            with jax.named_scope("q"):
                project_q((t + 3) // 2)

        return 0

    def scores(item, to):
        qc, g, src = item
        for i in range(group):
            to[i] = _dot(kv[g, src, 0], xq_s[:, pl.ds(pl.multiple_of(qc + i * HEAD, HEAD), HEAD)], 1, 1)

    def complete(t, g, p, slot, state, back):
        @pl.when((chip == last) & back)
        def _():
            i3 = back_index(g)
            with jax.named_scope("gotback"):
                for c in result_back(i3, me - CORES):
                    c.wait_recv()
            for i in range(group):
                mine, theirs = top_s[state, i : i + 1, :], st3[i3, i : i + 1, :]
                top = jnp.maximum(mine, theirs)
                a = jnp.exp2((mine - top) * E)
                b = jnp.exp2((theirs - top) * E) * st3[i3, group + i : group + i + 1, :]
                mix_s[state, i, :HEAD, :] = mix_s[state, i, :HEAD, :] * a + o3[i3, i].astype(F32) * b
                mix_s[state, i, HEAD:, :] = mix_s[state, i, HEAD:, :] * a + b

        for i in range(group):
            total = mix_s[state, i, HEAD : HEAD + 1, :]
            at = pl.ds(pl.multiple_of(t % 2 * gw + i * HEAD, HEAD), HEAD)
            o_s[:, at] = (mix_s[state, i, :HEAD, :] * (1 / total)).T.astype(BF16)

        def project(first, heads, out_ref):
            rows = slice(first * gw, (first + heads) * gw)
            for n in range(4):
                at = slice(n * wide, (n + 1) * wide)
                y = y_s[:, at] + _dot(o_s[:, rows], w_s[slot, n * pw + rows.start : n * pw + rows.stop, :wide], 1, 0)
                out_ref[:, at] = y.astype(out_ref.dtype)

        @pl.when((t % 2 == 1) & (t < kv_heads - 1))
        def _():
            with jax.named_scope("oproj"):
                for c in w_o(p, slot):
                    c.wait()
                project(0, 2, y_s)

            @pl.when(p < 2)
            def _():
                for c in w_o(2 * p + 1, 1):
                    c.start()

        @pl.when(t == kv_heads - 2)
        def _():
            for c in w_o(p, slot):
                c.wait()
            project(0, 1, y_s)

        @pl.when(t == kv_heads - 1)
        def _():
            with jax.named_scope("olast"):
                project(1, 1, y_ref)

    enter_diagonal(0)
    scores(item_diagonal(0), even_s)
    lax.fori_loop(-1, kv_heads, attend, 0)

    front = kv_heads - len(BACK)
    with jax.named_scope("drain"):
        sent(0, me, kv_heads)

        @pl.when(chip < before)
        def _():
            sent(1, me, kv_heads)

        @pl.when(chip == 0)
        def _():
            sent(2, me, kv_heads)

        def on(e, _):
            @pl.when(chip < last)
            def _():
                sent(0, e * CORES + core, kv_heads)

            @pl.when(chip == last)
            def _():
                sent(0, e * CORES + core, front)

            @pl.when(chip == before)
            def _():
                sent(1, e * CORES + core, front)

            return 0

        lax.fori_loop(0, chip, on, 0)

        @pl.when(chip == before)
        def _():
            sent(1, me, front)
            for i in range(len(BACK)):
                for c in result_back(i, me + CORES):
                    c.wait_send()

        @pl.when(chip == last)
        def _():
            for b in BACK:
                query_back(jnp.int32(b)).wait_send()


def rope_tables(T):
    half = HEAD // 2
    rate = float(THETA) ** (-np.arange(half) / half)
    sign = np.concatenate([-np.ones(half), np.ones(half)])

    def table(place):
        angle = np.tile(place[:, None] * rate, (1, 2))
        return np.cos(angle).astype(np.float32), (np.sin(angle) * sign).astype(np.float32)

    return np.concatenate(table(np.arange(SP) * T)), *table(np.arange(T))


def layer(x, gain, wq, wk, wv, wo):
    T, D = x.shape
    kv_heads = wk.shape[1] // HEAD
    group = wq.shape[1] // wk.shape[1]
    gw = group * HEAD
    pw = 2 * gw
    nb = len(BACK)
    dma = pltpu.SemaphoreType.DMA
    hbm, vmem = pl.BlockSpec(memory_space=pl.ANY), pl.BlockSpec(memory_space=pltpu.VMEM)
    flops = 2 * T * D * (2 * wq.shape[1] + 2 * wk.shape[1]) + 4 * T * T * SP * wq.shape[1] // 2
    return pl.pallas_call(
        functools.partial(_kernel, kv_heads=kv_heads, group=group),
        out_shape=pltpu.VMEM((T, D), BF16),
        in_specs=[hbm, vmem, vmem, hbm, hbm, hbm, hbm, hbm, hbm],
        out_specs=vmem,
        scratch_shapes=[
            pltpu.VMEM((T, max(D, (kv_heads + nb) * gw)), BF16),
            pltpu.VMEM((T, D), BF16),
            pltpu.VMEM((1, D), F32),
            pltpu.VMEM((T, HEAD), F32),
            pltpu.VMEM((T, HEAD), F32),
            pltpu.VMEM((2, D, 2 * HEAD), BF16),
            pltpu.VMEM((2, max(D, 4 * pw), max(pw, D // 4)), BF16),
            pltpu.VMEM((kv_heads, SP, 2, T, HEAD), BF16),
            pltpu.VMEM((nb, group, HEAD, T), BF16),
            pltpu.VMEM((nb, 8, T), F32),
            pltpu.VMEM((T, D), F32),
            pltpu.VMEM((T, pw), BF16),
            pltpu.VMEM((3, 8, T), F32),
            pltpu.VMEM((3, group, HEAD + 8, T), F32),
            pltpu.VMEM((group, T, T), F32),
            pltpu.VMEM((group, T, T), F32),
            dma((4,)), dma((2,)), dma((2, 2)), dma((2, 8)),
            dma((3, CHIPS)), dma((kv_heads, SP)), dma((nb,)), dma((nb,)), dma((2, nb)), dma((2, nb)),
        ],
        compiler_params=pltpu.CompilerParams(collective_id=0, has_side_effects=True, vmem_limit_bytes=VMEM),
        cost_estimate=pl.CostEstimate(flops=flops, transcendentals=T * T * SP * wq.shape[1] // HEAD, bytes_accessed=60 * 2**20),
    )(x, gain.reshape(D // HEAD, HEAD), *rope_tables(T), wq, wk, wv, wo)


def solution(mesh):
    tokens, whole = P(("dp", "sp"), None), P(None, None)
    return jax.shard_map(
        layer,
        mesh=mesh,
        in_specs=(tokens, P(None), whole, whole, whole, whole),
        out_specs=tokens,
        check_vma=False,
    )
```

```python
import functools

import jax
import jax.numpy as jnp
import numpy as np
from jax import lax
from jax.experimental import pallas as pl
from jax.experimental.pallas import tpu as pltpu
from jax.sharding import PartitionSpec as P

HEAD = 128
THETA = 10000
NEG = -1e30
HIDDEN = 2 * NEG
LOG2E = 1.4426950408889634
E = HEAD**-0.5 * LOG2E
VMEM = 60 * 2**20
BACK = (1, 3, 5, 7)
STEP = 16
CHIPS = 4
CORES = 2
SP = CHIPS * CORES
F32, BF16 = jnp.float32, jnp.bfloat16


def _dot(a, b, ca, cb):
    return lax.dot_general(a, b, (((ca,), (cb,)), ((), ())), preferred_element_type=F32)


def _kernel(x_ref, gain_ref, base_ref, cos_ref, sin_ref, wq_ref, wk_ref, wv_ref, wo_ref, y_ref,
            xq_s, a_s, gain_s, cos_s, sin_s, wkv_s, w_s, kv, o3, st3, y_s, top_s, mix_s, even_s, odd_s,
            x_sem, rope_sem, wkv_sem, w_sem, send_sem, recv_sem, qsend_sem, qrecv_sem, osend_sem, orecv_sem,
            *, kv_heads, group):
    T, D = x_ref.shape
    gw = group * HEAD
    pw = 2 * gw
    pairs = kv_heads // 2
    me = lax.axis_index("sp")
    chip, core = me // CORES, me % CORES
    other = me + 1 - 2 * core
    last, before = CHIPS - 1, CHIPS - 2

    def is_back(g):
        found = g == BACK[0]
        for b in BACK[1:]:
            found = found | (g == b)
        return found

    def back_index(g):
        return sum((g > b).astype(jnp.int32) for b in BACK)

    parts = 8
    rows = T // parts

    def x_part(i):
        at = pl.ds(i * rows, rows)
        return pltpu.make_async_copy(x_ref.at[at, :], xq_s.at[at, pl.ds(0, D)], x_sem.at[i])

    def ropes():
        return (pltpu.make_async_copy(cos_ref, cos_s, rope_sem.at[0]), pltpu.make_async_copy(sin_ref, sin_s, rope_sem.at[1]))

    def w_kv(g, slot):
        at = pl.ds(pl.multiple_of(g * HEAD, HEAD), HEAD)
        return (pltpu.make_async_copy(wk_ref.at[:, at], wkv_s.at[slot, :, pl.ds(0, HEAD)], wkv_sem.at[slot, 0]),
                pltpu.make_async_copy(wv_ref.at[:, at], wkv_s.at[slot, :, pl.ds(HEAD, HEAD)], wkv_sem.at[slot, 1]))

    def w_q(p, slot):
        return [w_q_part(p, slot, n) for n in range(4)]

    def w_q_part(p, slot, n):
        at = pl.ds(pl.multiple_of(n * (D // 4), HEAD), D // 4)
        return pltpu.make_async_copy(wq_ref.at[at, pl.ds(pl.multiple_of(p * pw, HEAD), pw)], w_s.at[slot, at, pl.ds(0, pw)],
                                     w_sem.at[slot, n])

    wide = D // 4

    def w_o(p, slot):
        at = [pl.ds(pl.multiple_of((2 * p + h) * gw, HEAD), gw) for h in range(2)]
        return [pltpu.make_async_copy(wo_ref.at[at[h], pl.ds(n * wide, wide)],
                                      w_s.at[slot, pl.ds(n * pw + h * gw, gw), pl.ds(0, wide)], w_sem.at[slot, 4 * h + n])
                for h in range(2) for n in range(4)]

    def piece(g, src, kind, target):
        return pltpu.make_async_remote_copy(src_ref=kv.at[g, src], dst_ref=kv.at[g, src], send_sem=send_sem.at[kind, src // CORES],
                                            recv_sem=recv_sem.at[g, src], device_id={"sp": target})

    def got(g, src):
        piece(g, src, 0, other).wait_recv()

    def q_at(g):
        return pl.ds(pl.multiple_of(g * gw, HEAD), gw)

    def query_back(g):
        i = back_index(g)
        return pltpu.make_async_remote_copy(src_ref=xq_s.at[:, q_at(g)], dst_ref=xq_s.at[:, q_at(kv_heads + i)], send_sem=qsend_sem.at[i],
                                            recv_sem=qrecv_sem.at[i], device_id={"sp": me - CORES})

    def result_back(i, target):
        return (pltpu.make_async_remote_copy(src_ref=o3.at[i], dst_ref=o3.at[i], send_sem=osend_sem.at[0, i],
                                             recv_sem=orecv_sem.at[0, i], device_id={"sp": target}),
                pltpu.make_async_remote_copy(src_ref=st3.at[i], dst_ref=st3.at[i], send_sem=osend_sem.at[1, i],
                                             recv_sem=orecv_sem.at[1, i], device_id={"sp": target}))

    def send_own(g):
        piece(g, me, 0, other).start()

        @pl.when((chip < before) | ((chip == before) & jnp.logical_not(is_back(g))))
        def _():
            piece(g, me, 1, me + CORES).start()

        @pl.when(chip == 0)
        def _():
            piece(g, me, 2, me + 2 * CORES).start()

    def send_on(g, src):
        piece(g, src, 0, other).start()

        @pl.when((chip == before) & jnp.logical_not(is_back(g)))
        def _():
            piece(g, src, 1, me + CORES).start()

    def sent(kind, src, heads):
        at = pl.ds(0, heads)
        pltpu.make_async_remote_copy(src_ref=kv.at[at, src], dst_ref=kv.at[at, src], send_sem=send_sem.at[kind, src // CORES],
                                     recv_sem=recv_sem.at[0, src], device_id={"sp": other}).wait_send()

    half_t = T // 2
    place = lax.broadcasted_iota(jnp.int32, (half_t, half_t), 1) - lax.broadcasted_iota(jnp.int32, (half_t, half_t), 0)

    for i in range(parts):
        x_part(i).start()
    barrier = pltpu.get_barrier_semaphore()
    for d in range(1, SP):
        pl.semaphore_signal(barrier, inc=1, device_id={"sp": lax.rem(me + d, SP)})
    for c in (*w_kv(0, 0), *ropes(), *w_kv(1, 1)):
        c.start()
    for n in range(D // HEAD):
        gain_s[:, n * HEAD : (n + 1) * HEAD] = gain_ref[n : n + 1, :].astype(F32)
    for i in range(parts):
        with jax.named_scope("waitx"):
            x_part(i).wait()
        step = min(rows, STEP)
        for at in range(i * rows, (i + 1) * rows, step):
            x = xq_s[at : at + step, :D].astype(F32)
            scale = lax.rsqrt(jnp.mean(x * x, -1, keepdims=True) + 1e-6)
            a_s[at : at + step, :] = (x * scale * gain_s[...]).astype(BF16)
    with jax.named_scope("rope"):
        for c in ropes():
            c.wait()
        cb, sb = base_ref[pl.ds(me, 1), :], base_ref[pl.ds(SP + me, 1), :]
        cr, sr = cos_s[...], sin_s[...]
        cos_s[...] = cr * cb - sr * sb
        sin_s[...] = sr * cb + cr * sb
    with jax.named_scope("bar"):
        pl.semaphore_wait(barrier, SP - 1)

    def turned(t):
        t = t.astype(BF16).astype(F32)
        return (t * cos_s[...] + pltpu.roll(t, HEAD // 2, 1) * sin_s[...]).astype(BF16)

    def project_kv(g, _):
        slot = g % 2
        with jax.named_scope("kvwait"):
            for c in w_kv(g, slot):
                c.wait()
        at = pl.ds(pl.multiple_of(g * (T // kv_heads), T // kv_heads), T // kv_heads)
        y_s[at, :] = xq_s[at, :D].astype(F32)
        r = _dot(a_s[...], wkv_s[slot], 1, 0)
        kv[g, me, 0] = turned(r[:, :HEAD])
        vt = r[:, HEAD:].T.astype(BF16)
        for n in range(T // HEAD):
            kv[g, me, 1, n * HEAD : (n + 1) * HEAD, :] = vt[:, n * HEAD : (n + 1) * HEAD]

        @pl.when(g + 2 < kv_heads)
        def _():
            for c in w_kv(g + 2, slot):
                c.start()

        @pl.when((g >= 3) & (g < 7))
        def _():
            w_q_part(0, 0, g - 3).start()

        send_own(g)
        return 0

    with jax.named_scope("kvall"):
        lax.fori_loop(0, kv_heads, project_kv, 0)

    def pass_on(g, e):
        src = e * CORES + core
        with jax.named_scope("gotremote"):
            got(g, src)
        send_on(g, src)

    def project_q(p):
        slot = jnp.where(p == 1, 1, 0)
        with jax.named_scope("qwait"):
            for c in w_q(p, slot):
                c.wait()
        r = _dot(a_s[...], w_s[slot, :D, :pw], 1, 0)
        for i in range(2 * group):
            xq_s[:, pl.ds(pl.multiple_of(p * pw + i * HEAD, HEAD), HEAD)] = turned(r[:, i * HEAD : (i + 1) * HEAD])

        for done, copies in ((0, lambda: w_q(2, 0)), (1, lambda: w_o(0, 1)), (2, lambda: w_q(3, 0)), (3, lambda: w_o(2, 0))):

            @pl.when(p == done)
            def _():
                for c in copies():
                    c.start()

        for h in range(2):
            g = 2 * p + h

            @pl.when((chip == last) & is_back(g))
            def _():
                query_back(g).start()

    for c in w_q(1, 1):
        c.start()
    with jax.named_scope("q0"):
        project_q(jnp.int32(0))

    def half(now, nxt, state, g, src, then, first=False, diagonal=False):
        qc, g_then, src_then = then
        keys = kv[g_then, src_then, 0]
        values = jnp.concatenate([kv[g, src, 1, n * HEAD : (n + 1) * HEAD, :] for n in range(T // HEAD)], axis=1)
        values = jnp.concatenate([values, jnp.ones((8, T), BF16)], axis=0)
        strip = T // 2 if diagonal else T
        for i in range(group):
            q = xq_s[:, pl.ds(pl.multiple_of(qc + i * HEAD, HEAD), HEAD)]
            for a in range(0, T, strip):
                at = slice(a, a + strip)
                nxt[i, :, at] = _dot(keys, q[at], 1, 1)
                end = a + strip if diagonal else T
                s = now[i, :end, at]
                if diagonal:
                    cut = jnp.where(place >= 0, s[a:], HIDDEN)
                    s = jnp.concatenate([s[:a], cut], axis=0) if a else cut
                top = s.max(axis=0, keepdims=True)
                if first:
                    top_s[state, i : i + 1, at] = top
                    mix_s[state, i, :, at] = _dot(values[:, :end], jnp.exp2((s - top) * E).astype(BF16), 1, 0)
                else:
                    old = top_s[state, i : i + 1, at]
                    top = jnp.maximum(old, top)
                    top_s[state, i : i + 1, at] = top
                    mix = _dot(values[:, :end], jnp.exp2((s - top) * E).astype(BF16), 1, 0)
                    mix_s[state, i, :, at] = mix_s[state, i, :, at] * jnp.exp2((old - top) * E) + mix

    def either(cond, a, b):
        return tuple(jnp.where(cond, x, y) for x, y in zip(a, b))

    def unit(state, g, qc, e, then):
        half(even_s, odd_s, state, g, e * CORES + core, (qc, g, e * CORES + 1 - core))
        half(odd_s, even_s, state, g, e * CORES + 1 - core, then)

    def is_guest(t):
        return (chip == before) & is_back(t) & (t >= 0) & (t < kv_heads)

    def own_units(t):
        n = jnp.where((chip == last) & is_back(t), 0, jnp.minimum(chip, last - 1))
        return jnp.where((t >= 0) & (t < kv_heads), n, 0)

    def units(t):
        return jnp.where(is_guest(t), 5, own_units(t))

    def unit_chip(t, k):
        return jnp.where(is_guest(t), last - 1 - (k + 1) // 2, own_units(t) - 1 - k)

    def for_guest(t, k):
        return is_guest(t) & ((k < 2) | (k == 3))

    def arriving(t, k):
        return jnp.logical_not(is_guest(t)) | (k == 1) | (k == 3)

    def column(t, k):
        g = t
        return jnp.where(for_guest(t, k), kv_heads + back_index(g), g) * gw

    def item_diagonal(t):
        g = t
        return g * gw, g, jnp.where(core == 1, other, me)

    def item_unit(t, k):
        return column(t, k), t, unit_chip(t, k) * CORES + core

    nothing = (jnp.int32(0), jnp.int32(0), me)

    def item_first(t):
        return either(t < kv_heads - 1, item_diagonal(t + 1), either(units(t) > 0, item_unit(t, 0), nothing))

    def enter_diagonal(t):
        with jax.named_scope("gotown"):
            got(t, other)

    def enter_unit(t, k):
        @pl.when(is_guest(t) & (k == 0))
        def _():
            with jax.named_scope("gotq3"):
                query_back(t).wait_recv()

        @pl.when(arriving(t, k))
        def _():
            pass_on(t, unit_chip(t, k))

    def enter_first(t):
        @pl.when(t < kv_heads - 1)
        def _():
            enter_diagonal(t + 1)

        @pl.when((t == kv_heads - 1) & (units(t) > 0))
        def _():
            enter_unit(t, 0)

    def enter_after_diagonal(t):
        @pl.when(units(t) > 0)
        def _():
            enter_unit(t, 0)

        @pl.when(units(t) == 0)
        def _():
            enter_first(t + 1)

    def attend(t, _):
        g = jnp.maximum(t, 0)
        p, state = t // 2, t % 2
        slot = jnp.where(p == 2, 0, 1)
        back = is_back(g)
        i3 = back_index(g)
        n = units(t)
        after_diagonal = either(n > 0, item_unit(t, 0), item_first(t + 1))

        @pl.when(t + 1 < kv_heads)
        def _():
            g1 = t + 1
            state1 = (t + 1) % 2
            near = (chip == last) & jnp.logical_not(is_back(g1))
            then = either(near, (g1 * gw, g1, (last - 1) * CORES + core), after_diagonal)

            @pl.when(near)
            def _():
                pass_on(g1, last - 1)

            @pl.when(jnp.logical_not(near))
            def _():
                enter_after_diagonal(t)

            @pl.when(core == 1)
            def _():
                with jax.named_scope("diag1"):
                    half(even_s, odd_s, state1, g1, other, (g1 * gw, g1, me), first=True)
                    half(odd_s, even_s, state1, g1, me, then, diagonal=True)

            @pl.when(core == 0)
            def _():
                with jax.named_scope("diag0"):
                    scores(item_diagonal(t + 1), odd_s)
                    half(odd_s, even_s, state1, g1, me, then, first=True, diagonal=True)

            @pl.when(near)
            def _():
                with jax.named_scope("gotother"):
                    got(g1, (last - 1) * CORES + 1 - core)
                enter_after_diagonal(t)
                with jax.named_scope("near"):
                    unit(state1, g1, g1 * gw, last - 1, after_diagonal)

        @pl.when(is_guest(t))
        def _():
            top_s[2] = jnp.full(top_s.shape[1:], NEG, F32)
            mix_s[2] = jnp.zeros(mix_s.shape[1:], F32)

        def rest(k, _):
            e = unit_chip(t, k)

            @pl.when(arriving(t, k))
            def _():
                with jax.named_scope("gotother"):
                    got(g, e * CORES + 1 - core)

            @pl.when(k + 1 < n)
            def _():
                enter_unit(t, k + 1)

            @pl.when(k + 1 == n)
            def _():
                enter_first(t + 1)

            with jax.named_scope("rest"):
                unit(jnp.where(for_guest(t, k), 2, state), g, column(t, k), e, either(k + 1 < n, item_unit(t, k + 1), item_first(t + 1)))

            @pl.when(is_guest(t) & (k == 3))
            def _():
                st3[i3, 0:group, :] = top_s[2, 0:group, :]
                for i in range(group):
                    total = mix_s[2, i, HEAD : HEAD + 1, :]
                    st3[i3, group + i : group + i + 1, :] = total
                    o3[i3, i] = (mix_s[2, i, :HEAD, :] * (1 / total)).astype(BF16)
                for c in result_back(i3, me + CORES):
                    c.start()

            return 0

        lax.fori_loop(0, n, rest, 0)

        @pl.when(t >= 0)
        def _():
            complete(t, g, p, slot, state, back)

        @pl.when((t % 2 == 1) & (t < 4))
        def _():
            with jax.named_scope("q"):
                project_q((t + 3) // 2)

        return 0

    def scores(item, to):
        qc, g, src = item
        for i in range(group):
            to[i] = _dot(kv[g, src, 0], xq_s[:, pl.ds(pl.multiple_of(qc + i * HEAD, HEAD), HEAD)], 1, 1)

    def complete(t, g, p, slot, state, back):
        @pl.when((chip == last) & back)
        def _():
            i3 = back_index(g)
            with jax.named_scope("gotback"):
                query_back(g).wait_send()
                for c in result_back(i3, me - CORES):
                    c.wait_recv()
            for i in range(group):
                mine, theirs = top_s[state, i : i + 1, :], st3[i3, i : i + 1, :]
                top = jnp.maximum(mine, theirs)
                a = jnp.exp2((mine - top) * E)
                b = jnp.exp2((theirs - top) * E) * st3[i3, group + i : group + i + 1, :]
                mix_s[state, i, :HEAD, :] = mix_s[state, i, :HEAD, :] * a + o3[i3, i].astype(F32) * b
                mix_s[state, i, HEAD:, :] = mix_s[state, i, HEAD:, :] * a + b

        for i in range(group):
            total = mix_s[state, i, HEAD : HEAD + 1, :]
            at = pl.ds(pl.multiple_of(g * gw + i * HEAD, HEAD), HEAD)
            xq_s[:, at] = (mix_s[state, i, :HEAD, :] * (1 / total)).T.astype(BF16)

        def project(p, slot, first, heads, out_ref):
            o = xq_s[:, pl.ds(pl.multiple_of(p * pw + first * gw, HEAD), heads * gw)]
            for n in range(4):
                at = slice(n * wide, (n + 1) * wide)
                rows = slice(n * pw + first * gw, n * pw + (first + heads) * gw)
                out_ref[:, at] = (y_s[:, at] + _dot(o, w_s[slot, rows, :wide], 1, 0)).astype(out_ref.dtype)

        def arrived(p, slot):
            for c in w_o(p, slot):
                c.wait()

        late = chip == before

        def pair(j, _):
            pj = jnp.where(late, jnp.where(t == kv_heads - 2, 0, 2 - j), t // 2)
            slot = jnp.where(pj == 2, 0, 1)
            with jax.named_scope("oproj"):
                arrived(pj, slot)
                project(pj, slot, 0, 2, y_s)

            @pl.when((late & (pj != 1)) | (jnp.logical_not(late) & (pj < 2)))
            def _():
                for c in w_o(jnp.where(pj == 0, 1, 3), slot):
                    c.start()

            return 0

        now = jnp.where(late, jnp.maximum(t - (kv_heads - 3), 0), jnp.where((t % 2 == 1) & (t < kv_heads - 1), 1, 0))
        lax.fori_loop(0, now, pair, 0)

        @pl.when((t == kv_heads - 2) & jnp.logical_not(late))
        def _():
            arrived(pairs - 1, 1)
            project(pairs - 1, 1, 0, 1, y_s)

        @pl.when((t == kv_heads - 1) & jnp.logical_not(late))
        def _():
            with jax.named_scope("olast"):
                project(pairs - 1, 1, 1, 1, y_ref)

        @pl.when((t == kv_heads - 1) & late)
        def _():
            with jax.named_scope("olast"):
                arrived(pairs - 1, 0)
                project(pairs - 1, 0, 0, 2, y_ref)

    enter_diagonal(0)
    scores(item_diagonal(0), even_s)
    lax.fori_loop(-1, kv_heads, attend, 0)

    front = kv_heads - len(BACK)
    with jax.named_scope("drain"):
        sent(0, me, kv_heads)

        @pl.when(chip < before)
        def _():
            sent(1, me, kv_heads)

        @pl.when(chip == 0)
        def _():
            sent(2, me, kv_heads)

        def on(e, _):
            @pl.when(chip < last)
            def _():
                sent(0, e * CORES + core, kv_heads)

            @pl.when(chip == last)
            def _():
                sent(0, e * CORES + core, front)

            @pl.when(chip == before)
            def _():
                sent(1, e * CORES + core, front)

            return 0

        lax.fori_loop(0, chip, on, 0)

        @pl.when(chip == before)
        def _():
            sent(1, me, front)
            for i in range(len(BACK)):
                for c in result_back(i, me + CORES):
                    c.wait_send()


def rope_tables(T):
    half = HEAD // 2
    rate = float(THETA) ** (-np.arange(half) / half)
    sign = np.concatenate([-np.ones(half), np.ones(half)])

    def table(place):
        angle = np.tile(place[:, None] * rate, (1, 2))
        return np.cos(angle).astype(np.float32), (np.sin(angle) * sign).astype(np.float32)

    return np.concatenate(table(np.arange(SP) * T)), *table(np.arange(T))


def layer(x, gain, wq, wk, wv, wo):
    T, D = x.shape
    kv_heads = wk.shape[1] // HEAD
    group = wq.shape[1] // wk.shape[1]
    gw = group * HEAD
    pw = 2 * gw
    nb = len(BACK)
    dma = pltpu.SemaphoreType.DMA
    hbm, vmem = pl.BlockSpec(memory_space=pl.ANY), pl.BlockSpec(memory_space=pltpu.VMEM)
    flops = 2 * T * D * (2 * wq.shape[1] + 2 * wk.shape[1]) + 4 * T * T * SP * wq.shape[1] // 2
    return pl.pallas_call(
        functools.partial(_kernel, kv_heads=kv_heads, group=group),
        out_shape=pltpu.VMEM((T, D), BF16),
        in_specs=[hbm, vmem, vmem, hbm, hbm, hbm, hbm, hbm, hbm],
        out_specs=vmem,
        scratch_shapes=[
            pltpu.VMEM((T, max(D, (kv_heads + nb) * gw)), BF16),
            pltpu.VMEM((T, D), BF16),
            pltpu.VMEM((1, D), F32),
            pltpu.VMEM((T, HEAD), F32),
            pltpu.VMEM((T, HEAD), F32),
            pltpu.VMEM((2, D, 2 * HEAD), BF16),
            pltpu.VMEM((2, max(D, 4 * pw), max(pw, D // 4)), BF16),
            pltpu.VMEM((kv_heads, SP, 2, T, HEAD), BF16),
            pltpu.VMEM((nb, group, HEAD, T), BF16),
            pltpu.VMEM((nb, 8, T), F32),
            pltpu.VMEM((T, D), F32),
            pltpu.VMEM((3, 8, T), F32),
            pltpu.VMEM((3, group, HEAD + 8, T), F32),
            pltpu.VMEM((group, T, T), F32),
            pltpu.VMEM((group, T, T), F32),
            dma((8,)), dma((2,)), dma((2, 2)), dma((2, 8)),
            dma((3, CHIPS)), dma((kv_heads, SP)), dma((nb,)), dma((nb,)), dma((2, nb)), dma((2, nb)),
        ],
        compiler_params=pltpu.CompilerParams(collective_id=0, has_side_effects=True, vmem_limit_bytes=VMEM),
        cost_estimate=pl.CostEstimate(flops=flops, transcendentals=T * T * SP * wq.shape[1] // HEAD, bytes_accessed=60 * 2**20),
    )(x, gain.reshape(D // HEAD, HEAD), *rope_tables(T), wq, wk, wv, wo)


def solution(mesh):
    tokens, whole = P(("dp", "sp"), None), P(None, None)
    return jax.shard_map(
        layer,
        mesh=mesh,
        in_specs=(tokens, P(None), whole, whole, whole, whole),
        out_specs=tokens,
        check_vma=False,
    )
```
